128 devices in a mesh: client: 32 (over z, x, core), head: 4 (over y).
Axes of the slice: x: 4, y: 4, z: 4, core: 2. Of those that a mesh axis runs over, the one named last changes fastest.
Arguments:
- pre: bfloat16 [40960, 4096], P('client'), may hold values from -40 to 40
- delta: float32 [40960, 4096], P('client', 'head'), may hold values from -300 to 300
- head_weight: bfloat16 [4096, 4096], P(None, 'head'), may hold values from -0.09375 to 0.09375
- client_ids: int32 [512], P('client'), may hold values from 0 to 511, as said below
Outputs:
- head_grad: float32 [4096, 4096], P('client', 'head')
- bias_grad: float32 [4096], P('head')
- embed_grad: float32 [512, 4096], P('client', 'head')
- span_grad: float32 [80, 4096], P(None, 'head')
The draws below stay inside these ranges and needn't reach their ends.
Inputs may be any that keep to these rules, and one draw needn't show every extreme that they name: `client_ids`: each of the 512 clients appears exactly once.
All inputs are finite; a program needn't handle non-finite values.
Results may differ from the reference program's by a relative error of at most 0.024.
Values may be sent and summed in bfloat16 or wider, within the bound.
A program may use at most 128 MiB of HBM per device.

```python
import jax
import jax.numpy as jnp
from jax import lax

HID = 4096
EMIT = 4096
SPANS = 80
CLIENTS = 512
ROWS = 40960
N_HEAD = 4


def shuffled_clients(key):
    return jax.random.permutation(jax.random.fold_in(key, 31), CLIENTS).astype(jnp.int32)


def draw_client_ids(key, part):
    return shuffled_clients(key)


def draw_pre(key, part):
    key_base = jax.random.fold_in(key, 11)
    key_level = jax.random.fold_in(key, 12)
    levels = jax.random.uniform(key_level, (HID,), jnp.float32, 0.0, 0.8)
    levels = levels + 0.48 * jnp.arange(HID, dtype=jnp.float32) / HID
    scales = 0.5 * 10.0 ** levels
    base = jnp.clip(jax.random.normal(key_base, (ROWS, HID), jnp.float32), -4.0, 4.0)
    return (base * scales[None, :]).astype(jnp.bfloat16)


def draw_delta(key, part):
    key_base = jax.random.fold_in(key, 21)
    key_rows = jax.random.fold_in(key, 22)
    key_cols = jax.random.fold_in(key, 23)
    owners = shuffled_clients(key).astype(jnp.float32) / CLIENTS
    col_levels = jax.random.uniform(key_cols, (EMIT,), jnp.float32, 0.0, 0.5)
    row_levels = jnp.repeat(owners, SPANS, total_repeat_length=ROWS)
    row_levels = row_levels + jax.random.uniform(key_rows, (ROWS,), jnp.float32, 0.0, 0.3)
    base = jnp.clip(jax.random.normal(key_base, (ROWS, EMIT), jnp.float32), -4.0, 4.0)
    values = base * (10.0 ** row_levels)[:, None] * (10.0 ** col_levels)[None, :]
    return values.astype(jnp.float32)


def shard_levels(stream_key, dims, shards, low, high):
    level, own = 1.0, jax.random.fold_in(stream_key, 6)
    for position, blocks in shards:
        heights = jnp.exp(jax.random.uniform(jax.random.fold_in(own, position), (blocks,), jnp.float32, low / len(shards), high / len(shards)))
        level = level * jnp.repeat(heights, dims[position] // blocks).reshape([-1 if axis == position else 1 for axis in range(len(dims))])
    return level


def gaussian(rng, shape, deviation, reach, cuts=(), kind=jnp.bfloat16):
    drawn = jax.random.normal(rng, shape, jnp.float32) * deviation
    if len(cuts) > 0:
        drawn = shard_levels(rng, shape, cuts, -0.22, 0.18) * drawn
    return jnp.clip(drawn, min=-reach, max=reach).astype(kind)


def setup_inputs(seed: int = 0) -> dict:
    key_of = jax.random.split(jax.random.key(seed), 5)
    pre = draw_pre(jax.random.fold_in(key_of[4], 71), 0)
    delta = draw_delta(jax.random.fold_in(key_of[4], 71), 0)
    head_weight = gaussian(key_of[2], (HID, EMIT), HID ** -0.5, 0.09375, ((1, 4),))
    client_ids = draw_client_ids(jax.random.fold_in(key_of[4], 71), 0)
    return {"pre": pre, "delta": delta, "head_weight": head_weight, "client_ids": client_ids}


def silu_slope(values):
    sigma = jax.nn.sigmoid(values)
    return sigma * (1.0 + values * (1.0 - sigma))

def clip_factor(total, number):
    return jnp.minimum(1.0, 1.0 / jnp.sqrt(total / number + 1e-06))

def reference(pre, delta, head_weight, client_ids):
    pre_wide = pre.astype(jnp.float32)
    hidden = jax.nn.silu(pre_wide).astype(jnp.bfloat16)
    delta_low = delta.astype(jnp.bfloat16)
    head_raw = jnp.dot(hidden.T, delta_low, preferred_element_type=jnp.float32)
    bias_raw = lax.optimization_barrier(jnp.sum(delta, axis=0))
    block = EMIT // N_HEAD
    hidden_grad = jnp.zeros((ROWS, HID), jnp.float32)
    for which in range(N_HEAD):
        partial_sum = jnp.dot(delta_low[:, which * block:(which + 1) * block], head_weight[:, which * block:(which + 1) * block].T, preferred_element_type=jnp.float32)
        rounded = lax.optimization_barrier(partial_sum.astype(jnp.bfloat16))
        hidden_grad = hidden_grad + rounded.astype(jnp.float32)
    pre_grad = hidden_grad * silu_slope(pre_wide)
    grouped = pre_grad.reshape(CLIENTS, SPANS, HID)
    client_part = lax.optimization_barrier(jnp.sum(grouped, axis=1))
    span_raw = lax.optimization_barrier(jnp.sum(grouped, axis=0))
    embed_raw = jnp.zeros((CLIENTS, HID), jnp.float32).at[client_ids.astype(jnp.int32)].add(client_part)
    head_factor = clip_factor(jnp.sum(head_raw * head_raw), HID * EMIT)
    embed_factor = clip_factor(jnp.sum(embed_raw * embed_raw), CLIENTS * HID)
    rest_total = jnp.sum(span_raw * span_raw) + jnp.sum(bias_raw * bias_raw)
    rest_factor = clip_factor(rest_total, SPANS * HID + EMIT)
    return (head_factor * head_raw, rest_factor * bias_raw, embed_factor * embed_raw, rest_factor * span_raw)
```

```python
import functools

import jax
import jax.numpy as jnp
from jax import lax
from jax.experimental import pallas as pl
from jax.experimental.pallas import tpu as pltpu
from jax.sharding import Mesh
from jax.sharding import PartitionSpec as P

CLIENT = ("client_0", "client_1", "client_2")
EPSILON = 1e-06
MESH = pl.DeviceIdType.MESH

ORDER = ((2, 2), (2, 1), (2, 3), (2, 0), (1, 2), (3, 2), (0, 2), (1, 1), (3, 1), (0, 1), (1, 3), (3, 3), (0, 3), (1, 0), (3, 0), (0, 0))
STEPS = 16
BLOCK = 256
LANES = 128
YORDER = (2, 1, 3, 0)


def digits(values):
    return sum(v * 4**i for i, v in enumerate(values))


def cut_along(x, dim, peers):
    before, after = (x.shape[:dim], x.shape[dim + 1 :])
    return jnp.moveaxis(x.reshape(*before, peers, -1, *after), dim, 0)


def sum_at_owner(x, axis, dim):
    tiles = cut_along(x, dim, lax.axis_size(axis))
    arrived = lax.all_to_all(tiles, axis, split_axis=0, concat_axis=0, tiled=True)
    return arrived.astype(jnp.float32).sum(axis=0)


def padded_to(lines, peers):
    spare = -len(lines) % peers
    return jnp.pad(lines, [(0, spare)] + [(0, 0)] * (lines.ndim - 1))


def joined_along(tiles, dim):
    shape = list(tiles.shape[1:])
    shape[dim] *= tiles.shape[0]
    return jnp.moveaxis(tiles, 0, dim).reshape(shape)


def sent_to_all(x, axis):
    peers = lax.axis_size(axis)
    return lax.all_to_all(jnp.broadcast_to(x[None], (peers, *x.shape)), axis, 0, 0, tiled=True)


def collect(x, axis, dim):
    return joined_along(sent_to_all(x, axis), dim)


def sum_by_parts(x, axes):
    lines = x.reshape(-1)
    padded = padded_to(lines, lax.axis_size(axes))
    whole = collect(sum_at_owner(padded, axes, 0).astype(jnp.bfloat16), axes, 0)
    return lax.slice_in_dim(whole, 0, len(lines)).reshape(x.shape).astype(jnp.float32)


def of_everyone(x, axis):
    return sent_to_all(x, axis).sum(axis=0)


def by_axis(x, axes):
    far, near = axes
    return of_everyone(of_everyone(x, near), far)


def in_one(arrays, axis):
    ends = [0]
    for a in arrays:
        ends.append(ends[-1] + a.size)
    subtotal = by_axis(jnp.concatenate([a.ravel() for a in arrays]), axis)
    return tuple((subtotal[b:e].reshape(a.shape) for a, b, e in zip(arrays, ends, ends[1:])))


def clip_factor(total, number):
    return jnp.minimum(1.0, 1.0 / jnp.sqrt(total / number + EPSILON))


def kernel(
    pre_hbm, delta_hbm, weight_hbm, head_out, sums_out, bias_out,
    stage, low, low_t, weight, pre_b, hid_a, hid_b, slope, prod, crecv, acc_a, acc_b, sums, sums_low, yrecv, r_a, r_b, r_a2, r_b2,
    delta_sem, weight_sem, pre_sem, c_send, c_recv, a_send, a_recv, b_send, b_recv, a2_send, a2_recv, b2_send, b2_recv, y_send, y_recv,
):
    rows = low.shape[0]
    clients = 16
    spans = rows // clients
    half = prod.shape[2] // 2
    z, x, c, y = (lax.axis_index(a) for a in (*CLIENT, "head"))

    def ring(one, offset):
        along_z = one * (1 - c) + (1 - one) * c
        return lax.rem(z + offset * along_z, 4), lax.rem(x + offset * (1 - along_z), 4), c, y

    partner = (z, x, 1 - c, y)
    barrier = pltpu.get_barrier_semaphore()
    others = [partner] + [ring(one, offset) for one in (1, 0) for offset in (1, 3)]
    others += [(z, x, c, lax.rem(y + offset, 4)) for offset in (1, 2, 3)]
    for other in others:
        pl.semaphore_signal(barrier, inc=1, device_id=other, device_id_type=MESH)

    def delta_copy(block):
        slot = block % 3
        return pltpu.make_async_copy(delta_hbm.at[pl.ds(block * 256, 256), :], stage.at[slot], delta_sem.at[slot])

    def chips(dp, dq):
        first = lax.rem(z + dp, 4) * 4 + lax.rem(x + dq, 4)
        second = lax.rem(z + dq, 4) * 4 + lax.rem(x + dp, 4)
        return first, second

    def pre_copies(dp, dq, slot):
        out = []
        for h, chip in enumerate(chips(dp, dq)):
            column = pl.multiple_of((chip * 2 + h) * LANES, LANES)
            out.append(
                pltpu.make_async_copy(
                    pre_hbm.at[:, pl.ds(column, LANES)],
                    pre_b.at[slot, :, pl.ds(h * LANES, LANES)],
                    pre_sem.at[slot, h],
                )
            )
        return out

    def weight_copy(part):
        size = weight.shape[0] // 4
        return pltpu.make_async_copy(weight_hbm.at[pl.ds(part * size, size), :], weight.at[pl.ds(part * size, size), :], weight_sem.at[part])

    def silu_to(slot, hid, at):
        for b in range(rows // 32):
            lines = pl.ds(b * 32, 32)
            v = pre_b[slot, lines, :].astype(jnp.float32)
            gate = 1.0 / (1.0 + jnp.exp(-v))
            value = v * gate
            hid[lines, :] = value.astype(jnp.bfloat16)
            slant = (gate + value * (1.0 - gate)).astype(jnp.bfloat16)
            for h in range(2):
                slope[at[h], lines, pl.ds(h * LANES, LANES)] = slant[:, h * LANES : (h + 1) * LANES]

    def remote(src, dst, send, recv, to):
        return pltpu.make_async_remote_copy(src_ref=src, dst_ref=dst, send_sem=send, recv_sem=recv, device_id=to, device_id_type=MESH)

    lower, upper = pl.ds(0, half), pl.ds(half, half)

    def core_copy(s):
        return remote(prod.at[s, 1 - c], crecv.at[s], c_send.at[s], c_recv.at[s], partner)

    def a_copies(i):
        return (
            remote(prod.at[i, c, lower], r_a.at[i, 0], a_send.at[i, 0], a_recv.at[i, 0], ring(1, 3)),
            remote(prod.at[i, c, upper], r_a.at[i, 1], a_send.at[i, 1], a_recv.at[i, 1], ring(1, 1)),
        )

    def b_copies(i):
        ahead, behind = 4 + 3 * i, 5 + 3 * i

        def one(chunk, part, side, k, to):
            return remote(prod.at[chunk, c, part], r_b.at[i, side, part], b_send.at[i, k], b_recv.at[i, k], to)

        return (
            one(ahead, lower, 0, 0, ring(1, 1)),
            one(behind, upper, 1, 1, ring(1, 3)),
            one(ahead, upper, 0, 2, ring(1, 1)),
            one(behind, lower, 1, 3, ring(1, 3)),
        )

    def a2_copies():
        chunk = 6
        return (
            remote(prod.at[chunk, c, lower], r_a2.at[0], a2_send.at[0], a2_recv.at[0], ring(0, 3)),
            remote(prod.at[chunk, c, upper], r_a2.at[1], a2_send.at[1], a2_recv.at[1], ring(0, 1)),
        )

    def b2_copies():
        def one(chunk, part, side, k, to):
            return remote(prod.at[chunk, c, part], r_b2.at[side, part], b2_send.at[k], b2_recv.at[k], to)

        return (
            one(9, lower, 0, 0, ring(0, 1)),
            one(12, upper, 1, 1, ring(0, 3)),
            one(9, upper, 0, 2, ring(0, 1)),
            one(12, lower, 1, 3, ring(0, 3)),
        )

    def core_add(s):
        core_copy(s).wait_recv()
        prod[s, c] = prod[s, c] + crecv[s]

    def do_a(i):
        for copy in a_copies(i):
            copy.start()

    def do_b(i):
        first, second, third, fourth = b_copies(i)
        first.start()
        second.start()
        from_plus, from_minus = a_copies(i)
        ahead, behind = 4 + 3 * i, 5 + 3 * i
        from_minus.wait_recv()
        prod[ahead, c, upper] = prod[ahead, c, upper] + r_a[i, 1]
        from_plus.wait_recv()
        prod[behind, c, lower] = prod[behind, c, lower] + r_a[i, 0]
        third.start()
        fourth.start()

    def three(a, b, d):
        return a.astype(jnp.float32) + b.astype(jnp.float32) + d.astype(jnp.float32)

    def do_f(i):
        for copy in b_copies(i):
            copy.wait_recv()
        chunk = 6 + 3 * i
        prod[chunk, c] = three(prod[chunk, c], r_b[i, 0], r_b[i, 1]).astype(jnp.bfloat16)

    def do_a2():
        for copy in a2_copies():
            copy.start()

    def do_b2():
        first, second, third, fourth = b2_copies()
        first.start()
        second.start()
        from_plus, from_minus = a2_copies()
        from_minus.wait_recv()
        prod[9, c, upper] = prod[9, c, upper] + r_a2[1]
        from_plus.wait_recv()
        prod[12, c, lower] = prod[12, c, lower] + r_a2[0]
        third.start()
        fourth.start()

    def do_final():
        for copy in b2_copies():
            copy.wait_recv()
        whole = three(prod[15, c], r_b2[0], r_b2[1])
        head_out[...] = whole.T

    def y_copy(group):
        to = lax.rem(y + jnp.int32(0) + offset_of(group), 4)
        return remote(
            sums_low.at[pl.ds(4 * group, 4)], yrecv.at[group], y_send.at[group], y_recv.at[group], (z, x, c, to)
        )

    def offset_of(group):
        return YORDER[group]

    for block in range(3):
        delta_copy(block).start()
    for s in range(4):
        for copy in pre_copies(*ORDER[s], s):
            copy.start()
    bias = jnp.zeros((1, low.shape[1]), jnp.float32)
    for block in range(rows // 256):
        delta_copy(block).wait()
        lines = pl.ds(block * 256, 256)
        values = stage[block % 3]
        bias = bias + jnp.sum(values, axis=0, keepdims=True)
        rounded = values.astype(jnp.bfloat16)
        low[lines, :] = rounded
        low_t[:, lines] = rounded.T
        if block + 3 < rows // 256:
            delta_copy(block + 3).start()
    bias_out[...] = bias
    for part in range(4):
        weight_copy(part).start()
    for copy in pre_copies(*ORDER[0], 0):
        copy.wait()
    silu_to(0, hid_a, chips(*ORDER[0]))
    for copy in pre_copies(*ORDER[4], 0):
        copy.start()
    pl.semaphore_wait(barrier, len(others))

    next_p, next_q = digits([o[0] for o in ORDER[1:]]), digits([o[1] for o in ORDER[1:]])
    load_p, load_q = digits([o[0] for o in ORDER[5:]]), digits([o[1] for o in ORDER[5:]])

    def first_product(i, carry):
        np_, nq_, lp_, lq_ = carry
        for k, (now, later) in enumerate(((hid_a, hid_b), (hid_b, hid_a))):
            s = 2 * i + k
            slot = lax.rem(s + 1, 4)
            dp, dq = lax.rem(np_, 4), lax.rem(nq_, 4)

            @pl.when(s < STEPS - 1)
            def _():
                for copy in pre_copies(dp, dq, slot):
                    copy.wait()

            last = lax.div(s, STEPS - 1)
            at = [chip * (1 - last) + STEPS * last for chip in chips(dp, dq)]
            silu_to(slot, later, at)
            product = jnp.dot(low_t[...], now[...], preferred_element_type=jnp.float32).astype(jnp.bfloat16)
            for h in range(2):
                prod[s, h] = product[:, h * LANES : (h + 1) * LANES]

            @pl.when(s + 5 < STEPS)
            def _():
                for copy in pre_copies(lax.rem(lp_, 4), lax.rem(lq_, 4), slot):
                    copy.start()

            core_copy(s).start()

            @pl.when(s >= 2)
            def _():
                core_add(s - 2)

            if k == 0:
                pl.when(i == 1)(lambda: do_a(0))
                pl.when(i == 2)(lambda: do_a(2))
                pl.when(i == 5)(lambda: do_b(1))
            else:
                pl.when(i == 1)(lambda: do_a(1))
                pl.when(i == 2)(lambda: do_a(3))
                pl.when(i == 3)(lambda: do_b(0))
                pl.when(i == 6)(lambda: do_b(2))

                @pl.when(i == 7)
                def _():
                    do_f(0)
                    do_a2()

            np_, nq_, lp_, lq_ = (lax.div(t, 4) for t in (np_, nq_, lp_, lq_))
        return np_, nq_, lp_, lq_

    lax.fori_loop(0, STEPS // 2, first_product, tuple(jnp.int32(t) for t in (next_p, next_q, load_p, load_q)))

    def reduce_rows(acc, chunk, u):
        span = jnp.zeros((spans, BLOCK), jnp.float32)
        for client in range(clients):
            lines = pl.ds(client * spans, spans)
            grad = acc[lines, :] * slope[chunk, lines, :].astype(jnp.float32)
            span = span + grad
            whole = jnp.sum(grad, axis=0, keepdims=True)
            sums[u, pl.ds(spans + client, 1), :] = whole
        sums[u, pl.ds(0, spans), :] = span
        sums_low[u] = sums[u].astype(jnp.bfloat16)

    for part in range(4):
        weight_copy(part).wait()

    def second_product(g, carry):
        before, table = carry
        chunk0 = lax.rem(y + lax.rem(table, 4), 4) * 4
        for t in range(4):
            u = 4 * g + t
            now, last = (acc_a, acc_b) if t % 2 == 0 else (acc_b, acc_a)
            chunk = chunk0 + t
            previous = before if t == 0 else chunk - 1
            slot = lax.rem(u + STEPS, STEPS + 1)
            reduce_rows(last, previous, slot)
            lines = pl.ds(pl.multiple_of(chunk * BLOCK, BLOCK), BLOCK)
            now[...] = lax.dot_general(low[...], weight[lines, :], (((1,), (1,)), ((), ())), preferred_element_type=jnp.float32)
            if t == 0:

                @pl.when(g == 0)
                def _():
                    core_add(STEPS - 2)
                    do_b(3)

                @pl.when(g == 3)
                def _():
                    do_final()

                for group in range(3):
                    pl.when(g == group + 1)(lambda group=group: y_copy(group).start())
            elif t == 1:

                @pl.when(g == 0)
                def _():
                    core_add(STEPS - 1)

            elif t == 2:

                pl.when(g == 0)(lambda: do_f(1))

                @pl.when(g == 1)
                def _():
                    do_f(2)
                    do_b2()

                pl.when(g == 2)(lambda: do_f(3))
        return chunk0 + 3, lax.div(table, 4)

    final_chunk, _ = lax.fori_loop(0, 4, second_product, (jnp.int32(0), jnp.int32(digits(YORDER))))
    reduce_rows(acc_b, final_chunk, STEPS - 1)
    for group in range(3):
        y_copy(group).wait_recv()
    for t in range(4):
        total = sums[12 + t]
        for group in range(3):
            total = total + yrecv[group, t].astype(jnp.float32)
        sums_out[:, pl.ds(t * BLOCK, BLOCK)] = total

    def all_sent(s, _):
        core_copy(s).wait_send()
        return 0

    lax.fori_loop(0, STEPS, all_sent, 0)
    for i in range(4):
        for copy in (*a_copies(i), *b_copies(i)):
            copy.wait_send()
    for copy in (*a2_copies(), *b2_copies()):
        copy.wait_send()
    for group in range(3):
        y_copy(group).wait_send()


def local_products(pre, delta, head_weight):
    rows, width = pre.shape
    here = delta.shape[1]
    bf16, f32 = jnp.bfloat16, jnp.float32
    dma = pltpu.SemaphoreType.DMA
    spans = rows // 16
    anywhere = pl.BlockSpec(memory_space=pl.ANY)
    in_vmem = pl.BlockSpec(memory_space=pltpu.VMEM)
    return pl.pallas_call(
        kernel,
        name="products",
        out_shape=(
            jax.ShapeDtypeStruct((LANES, here), f32),
            jax.ShapeDtypeStruct((spans + 16, here), f32),
            jax.ShapeDtypeStruct((1, here), f32),
        ),
        in_specs=[anywhere] * 3,
        out_specs=[in_vmem] * 3,
        scratch_shapes=[
            pltpu.VMEM((3, 256, here), f32),
            pltpu.VMEM((rows, here), bf16),
            pltpu.VMEM((here, rows), bf16),
            pltpu.VMEM((width, here), bf16),
            pltpu.VMEM((4, rows, BLOCK), bf16),
            pltpu.VMEM((rows, BLOCK), bf16),
            pltpu.VMEM((rows, BLOCK), bf16),
            pltpu.VMEM((STEPS + 1, rows, BLOCK), bf16),
            pltpu.VMEM((STEPS, 2, here, LANES), bf16),
            pltpu.VMEM((STEPS, here, LANES), bf16),
            pltpu.VMEM((rows, BLOCK), f32),
            pltpu.VMEM((rows, BLOCK), f32),
            pltpu.VMEM((STEPS + 1, spans + 16, BLOCK), f32),
            pltpu.VMEM((STEPS + 1, spans + 16, BLOCK), bf16),
            pltpu.VMEM((3, 4, spans + 16, BLOCK), bf16),
            pltpu.VMEM((4, 2, here // 2, LANES), bf16),
            pltpu.VMEM((4, 2, here, LANES), bf16),
            pltpu.VMEM((2, here // 2, LANES), bf16),
            pltpu.VMEM((2, here, LANES), bf16),
            dma((3,)),
            dma((4,)),
            dma((4, 2)),
            dma((STEPS,)),
            dma((STEPS,)),
            dma((4, 2)),
            dma((4, 2)),
            dma((4, 4)),
            dma((4, 4)),
            dma((2,)),
            dma((2,)),
            dma((4,)),
            dma((4,)),
            dma((3,)),
            dma((3,)),
        ],
        compiler_params=pltpu.CompilerParams(collective_id=0, has_side_effects=True, vmem_limit_bytes=67_000_000),
    )(pre, delta, head_weight)


def per_device(pre, delta, head_weight, client_ids):
    rows_here, hidden_width = pre.shape
    emit_here = delta.shape[1]
    clients_here = client_ids.shape[0]
    span_count = rows_here // clients_here
    head_devices = lax.axis_size("head")
    client_devices = lax.axis_size(CLIENT)
    head_raw, sums, bias = local_products(pre, delta, head_weight)
    head_square = jnp.sum(head_raw * head_raw)
    span_part, client_part, bias_local = sums[:span_count], sums[span_count:], bias[0]
    span_raw, bias_raw = (
        sum_by_parts(span_part.astype(jnp.bfloat16), CLIENT),
        sum_by_parts(bias_local.astype(jnp.bfloat16), CLIENT),
    )
    targets = lax.iota(jnp.int32, clients_here * lax.axis_size(CLIENT))
    selector = (targets[:, None] == client_ids[None, :]).astype(jnp.float32)
    embed_raw = sum_at_owner(
        jnp.dot(
            selector,
            client_part,
            precision=lax.Precision.HIGHEST,
            preferred_element_type=jnp.float32,
        ).astype(jnp.bfloat16),
        CLIENT,
        0,
    )
    leading = (lax.axis_index(CLIENT) == 0).astype(jnp.float32)
    small_square = leading * (jnp.sum(span_raw * span_raw) + jnp.sum(bias_raw * bias_raw))
    embed_square = jnp.sum(embed_raw * embed_raw)
    head_total, embed_total, small_total = in_one(
        (head_square, embed_square, small_square), (("client_0", "client_1"), ("client_2", "head"))
    )
    emit_total = emit_here * head_devices
    clients_total = clients_here * client_devices
    head_factor = clip_factor(head_total, hidden_width * emit_total)
    embed_factor = clip_factor(embed_total, clients_total * hidden_width)
    rest_factor = clip_factor(small_total, span_count * hidden_width + emit_total)
    return (
        head_factor * head_raw,
        rest_factor * bias_raw,
        embed_factor * embed_raw,
        rest_factor * span_raw,
    )


def solution(mesh):
    torus = Mesh(
        mesh.devices.reshape(4, 4, 2, mesh.shape["head"]),
        ("client_0", "client_1", "client_2", "head"),
    )
    return jax.shard_map(
        per_device,
        mesh=torus,
        in_specs=(P(CLIENT, None), P(CLIENT, "head"), P(None, "head"), P(CLIENT)),
        out_specs=(P(CLIENT, "head"), P("head"), P(CLIENT, "head"), P(None, "head")),
        check_vma=False,
    )
```

```python
import jax
import jax.numpy as jnp
from jax import lax
from jax.experimental import pallas as pl
from jax.experimental.pallas import tpu as pltpu
from jax.sharding import Mesh
from jax.sharding import PartitionSpec as P

CLIENT = ("client_0", "client_1", "client_2")
EPSILON = 1e-06
MESH = pl.DeviceIdType.MESH

ORDER = ((2, 2), (2, 1), (2, 3), (2, 0), (1, 2), (3, 2), (0, 2), (1, 1), (3, 1), (0, 1), (1, 3), (3, 3), (0, 3), (1, 0), (3, 0), (0, 0))
STEPS = 16
BLOCK = 256
LANES = 128
YORDER = (2, 1, 3, 0)


def digits(values):
    return sum(v * 4**i for i, v in enumerate(values))


def kernel(
    pre_hbm, delta_hbm, weight_hbm, ids_ref, head_out, bias_out, embed_out, span_out,
    stage, low, low_t, weight, pre_b, hid_a, hid_b, slope, prod, crecv, acc_a, acc_b, sums, sums_low, yrecv, r_a, r_b, r_a2, r_b2,
    ids, emb, rest_own, rest_in, rest_all, picked, picked_in, squares, squares_zx, squares_y,
    delta_sem, weight_sem, pre_sem, c_send, c_recv, a_send, a_recv, b_send, b_recv, a2_send, a2_recv, b2_send, b2_recv, y_send, y_recv,
    i_send, i_recv, e_send, e_recv, rs_send, rs_recv, ag_send, ag_recv, p_send, p_recv, zx_send, zx_recv, sy_send, sy_recv,
):
    rows = low.shape[0]
    here = low.shape[1]
    clients = 16
    spans = rows // clients
    half = prod.shape[2] // 2
    z, x, c, y = (lax.axis_index(a) for a in (*CLIENT, "head"))

    def ring(one, offset):
        along_z = one * (1 - c) + (1 - one) * c
        return lax.rem(z + offset * along_z, 4), lax.rem(x + offset * (1 - along_z), 4), c, y

    def client_peer(o):
        return lax.rem(z + lax.div(o, 8), 4), lax.rem(x + lax.rem(lax.div(o, 2), 4), 4), lax.rem(c + lax.rem(o, 2), 2), y

    def plane_peer(o):
        return lax.rem(z + lax.div(o, 4), 4), lax.rem(x + lax.rem(o, 4), 4), c, y

    def column_peer(o):
        return z, x, lax.rem(c + lax.rem(o, 2), 2), lax.rem(y + lax.div(o, 2), 4)

    partner = (z, x, 1 - c, y)
    barrier = pltpu.get_barrier_semaphore()

    def greet(peer, first, last):
        def one(o, carry):
            pl.semaphore_signal(barrier, inc=1, device_id=peer(o), device_id_type=MESH)
            return carry

        lax.fori_loop(first, last, one, 0)

    greet(client_peer, 1, 32)
    greet(column_peer, 2, 8)

    def delta_copy(block):
        slot = block % 3
        return pltpu.make_async_copy(delta_hbm.at[pl.ds(block * 256, 256), :], stage.at[slot], delta_sem.at[slot])

    def chips(dp, dq):
        first = lax.rem(z + dp, 4) * 4 + lax.rem(x + dq, 4)
        second = lax.rem(z + dq, 4) * 4 + lax.rem(x + dp, 4)
        return first, second

    def pre_copies(dp, dq, slot):
        out = []
        for h, chip in enumerate(chips(dp, dq)):
            column = pl.multiple_of((chip * 2 + h) * LANES, LANES)
            out.append(
                pltpu.make_async_copy(
                    pre_hbm.at[:, pl.ds(column, LANES)],
                    pre_b.at[slot, :, pl.ds(h * LANES, LANES)],
                    pre_sem.at[slot, h],
                )
            )
        return out

    def weight_copy(part):
        size = weight.shape[0] // 4
        return pltpu.make_async_copy(weight_hbm.at[pl.ds(part * size, size), :], weight.at[pl.ds(part * size, size), :], weight_sem.at[part])

    def silu_to(slot, hid, at):
        for b in range(rows // 32):
            lines = pl.ds(b * 32, 32)
            v = pre_b[slot, lines, :].astype(jnp.float32)
            gate = 1.0 / (1.0 + jnp.exp(-v))
            value = v * gate
            hid[lines, :] = value.astype(jnp.bfloat16)
            slant = (gate + value * (1.0 - gate)).astype(jnp.bfloat16)
            for h in range(2):
                slope[at[h], lines, pl.ds(h * LANES, LANES)] = slant[:, h * LANES : (h + 1) * LANES]

    def remote(src, dst, send, recv, to):
        return pltpu.make_async_remote_copy(src_ref=src, dst_ref=dst, send_sem=send, recv_sem=recv, device_id=to, device_id_type=MESH)

    lower, upper = pl.ds(0, half), pl.ds(half, half)

    def core_copy(s):
        return remote(prod.at[s, 1 - c], crecv.at[s], c_send.at[s], c_recv.at[s], partner)

    def a_copies(i):
        return (
            remote(prod.at[i, c, lower], r_a.at[i, 0], a_send.at[i, 0], a_recv.at[i, 0], ring(1, 3)),
            remote(prod.at[i, c, upper], r_a.at[i, 1], a_send.at[i, 1], a_recv.at[i, 1], ring(1, 1)),
        )

    def b_copies(i):
        ahead, behind = 4 + 3 * i, 5 + 3 * i

        def one(chunk, part, side, k, to):
            return remote(prod.at[chunk, c, part], r_b.at[i, side, part], b_send.at[i, k], b_recv.at[i, k], to)

        return (
            one(ahead, lower, 0, 0, ring(1, 1)),
            one(behind, upper, 1, 1, ring(1, 3)),
            one(ahead, upper, 0, 2, ring(1, 1)),
            one(behind, lower, 1, 3, ring(1, 3)),
        )

    def a2_copies():
        chunk = 6
        return (
            remote(prod.at[chunk, c, lower], r_a2.at[0], a2_send.at[0], a2_recv.at[0], ring(0, 3)),
            remote(prod.at[chunk, c, upper], r_a2.at[1], a2_send.at[1], a2_recv.at[1], ring(0, 1)),
        )

    def b2_copies():
        def one(chunk, part, side, k, to):
            return remote(prod.at[chunk, c, part], r_b2.at[side, part], b2_send.at[k], b2_recv.at[k], to)

        return (
            one(9, lower, 0, 0, ring(0, 1)),
            one(12, upper, 1, 1, ring(0, 3)),
            one(9, upper, 0, 2, ring(0, 1)),
            one(12, lower, 1, 3, ring(0, 3)),
        )

    def y_copy(group):
        to = lax.rem(y + YORDER[group], 4)
        return remote(sums_low.at[pl.ds(4 * group, 4)], yrecv.at[group], y_send.at[group], y_recv.at[group], (z, x, c, to))

    def id_copies(stage_):
        if stage_ == 0:
            return [remote(ids.at[0, 0], ids.at[0, o], i_send.at[0, o], i_recv.at[0, o], ring(1, o)) for o in (2, 1, 3)]
        return [remote(ids.at[0], ids.at[o], i_send.at[1, o], i_recv.at[1, o], ring(0, o)) for o in (2, 1, 3)]

    def embed_copies(stage_):
        if stage_ == 0:
            return [remote(emb.at[0, 0], emb.at[0, o], e_send.at[0, o], e_recv.at[0, o], ring(1, o)) for o in (2, 1, 3)]
        return [remote(emb.at[0], emb.at[o], e_send.at[1, o], e_recv.at[1, o], ring(0, o)) for o in (2, 1, 3)]

    def piece_of(zz, xx, cc):
        return pl.ds(pl.multiple_of(zz * 32, 32), 32), pl.ds(pl.multiple_of((xx * 2 + cc) * LANES, LANES), LANES)

    def scatter_copy(o):
        to = client_peer(o)
        return remote(rest_own.at[piece_of(*to[:3])], rest_in.at[o], rs_send.at[o], rs_recv.at[o], to)

    def gather_copy(o):
        mine = piece_of(z, x, c)
        return remote(rest_all.at[mine], rest_all.at[mine], ag_send.at[o], ag_recv.at[o], client_peer(o))

    def picked_copy():
        return remote(picked, picked_in, p_send.at[0], p_recv.at[0], partner)

    def plane_copy(o):
        return remote(squares.at[0], squares_zx.at[o], zx_send.at[o], zx_recv.at[o], plane_peer(o))

    def column_copy(o):
        return remote(squares.at[1], squares_y.at[o], sy_send.at[o], sy_recv.at[o], column_peer(o))

    def over(first, last, what):
        def one(o, carry):
            what(o)
            return carry

        lax.fori_loop(first, last, one, 0)

    def start_all(copies):
        for copy in copies:
            copy.start()

    def arrive_all(copies):
        for copy in copies:
            copy.wait_recv()

    def core_add(s):
        core_copy(s).wait_recv()
        prod[s, c] = prod[s, c] + crecv[s]

    def do_b(i):
        first, second, third, fourth = b_copies(i)
        first.start()
        second.start()
        from_plus, from_minus = a_copies(i)
        ahead, behind = 4 + 3 * i, 5 + 3 * i
        from_minus.wait_recv()
        prod[ahead, c, upper] = prod[ahead, c, upper] + r_a[i, 1]
        from_plus.wait_recv()
        prod[behind, c, lower] = prod[behind, c, lower] + r_a[i, 0]
        third.start()
        fourth.start()

    def three(a, b, d):
        return a.astype(jnp.float32) + b.astype(jnp.float32) + d.astype(jnp.float32)

    def do_f(i):
        arrive_all(b_copies(i))
        chunk = 6 + 3 * i
        prod[chunk, c] = three(prod[chunk, c], r_b[i, 0], r_b[i, 1]).astype(jnp.bfloat16)

    def do_b2():
        first, second, third, fourth = b2_copies()
        first.start()
        second.start()
        from_plus, from_minus = a2_copies()
        from_minus.wait_recv()
        prod[9, c, upper] = prod[9, c, upper] + r_a2[1]
        from_plus.wait_recv()
        prod[12, c, lower] = prod[12, c, lower] + r_a2[0]
        third.start()
        fourth.start()

    def do_final():
        arrive_all(b2_copies())
        whole = three(prod[15, c], r_b2[0], r_b2[1])
        squares[0, pl.ds(0, 1), :] = jnp.sum(whole * whole, axis=0, keepdims=True)
        head_out[...] = whole.T

    start_all(pre_copies(*ORDER[0], 0))
    for block in range(3):
        delta_copy(block).start()
    for s in range(1, 4):
        start_all(pre_copies(*ORDER[s], s))
    for client in range(clients):
        ids[0, 0, pl.ds(client, 1), :] = jnp.full((1, LANES), ids_ref[client], jnp.int32)
    squares[...] = jnp.zeros(squares.shape, jnp.float32)
    rest_own[pl.ds(96, 32), :] = jnp.zeros((32, here), jnp.bfloat16)
    for copy in pre_copies(*ORDER[0], 0):
        copy.wait()
    silu_to(0, hid_a, chips(*ORDER[0]))
    start_all(pre_copies(*ORDER[4], 0))
    bias = jnp.zeros((1, here), jnp.float32)
    for block in range(rows // 256):
        delta_copy(block).wait()
        lines = pl.ds(block * 256, 256)
        values = stage[block % 3]
        bias = bias + jnp.sum(values, axis=0, keepdims=True)
        rounded = values.astype(jnp.bfloat16)
        low[lines, :] = rounded
        low_t[:, lines] = rounded.T
        if block + 3 < rows // 256:
            delta_copy(block + 3).start()
    first_line = lax.broadcasted_iota(jnp.int32, (16, here), 0) == 0
    rest_own[pl.ds(80, 16), :] = jnp.where(first_line, jnp.broadcast_to(bias, (16, here)), 0.0).astype(jnp.bfloat16)
    for part in range(4):
        weight_copy(part).start()
    pl.semaphore_wait(barrier, 37)
    start_all(id_copies(0))

    next_p, next_q = digits([o[0] for o in ORDER[1:]]), digits([o[1] for o in ORDER[1:]])
    load_p, load_q = digits([o[0] for o in ORDER[5:]]), digits([o[1] for o in ORDER[5:]])

    def first_product(i, carry):
        np_, nq_, lp_, lq_ = carry
        offsets, slots = [], []
        for k in range(2):
            offsets.append((lax.rem(np_, 4), lax.rem(nq_, 4)))
            slots.append(lax.rem(2 * i + k + 1, 4))
            np_, nq_ = lax.div(np_, 4), lax.div(nq_, 4)

        def arrived(k):
            for copy in pre_copies(*offsets[k], slots[k]):
                copy.wait()

        arrived(0)
        pl.when(i < STEPS // 2 - 1)(lambda: arrived(1))
        last = lax.div(i, STEPS // 2 - 1)
        for k, (now, later) in enumerate(((hid_a, hid_b), (hid_b, hid_a))):
            s = 2 * i + k
            spare = last if k == 1 else 0
            at = [chip * (1 - spare) + STEPS * spare for chip in chips(*offsets[k])]
            silu_to(slots[k], later, at)
            product = jnp.dot(low_t[...], now[...], preferred_element_type=jnp.float32).astype(jnp.bfloat16)
            for h in range(2):
                prod[s, h] = product[:, h * LANES : (h + 1) * LANES]

        core_copy(2 * i).start()
        core_copy(2 * i + 1).start()
        for k in range(2):

            @pl.when(2 * i + k + 5 < STEPS)
            def _(k=k, lp_=lp_, lq_=lq_):
                start_all(pre_copies(lax.rem(lp_, 4), lax.rem(lq_, 4), slots[k]))

            lp_, lq_ = lax.div(lp_, 4), lax.div(lq_, 4)

        @pl.when(i == 0)
        def _():
            arrive_all(id_copies(0))
            start_all(id_copies(1))

        @pl.when(i >= 1)
        def _():
            core_add(2 * i - 2)
            core_add(2 * i - 1)

        @pl.when(i == 1)
        def _():
            start_all(a_copies(0))
            start_all(a_copies(1))

        @pl.when(i == 2)
        def _():
            start_all(a_copies(2))
            start_all(a_copies(3))

        pl.when(i == 3)(lambda: do_b(0))
        pl.when(i == 5)(lambda: do_b(1))

        @pl.when(i == 6)
        def _():
            do_b(2)
            do_f(0)
            start_all(a2_copies())

        return np_, nq_, lp_, lq_

    lax.fori_loop(0, STEPS // 2, first_product, tuple(jnp.int32(t) for t in (next_p, next_q, load_p, load_q)))

    def reduce_rows(acc, chunk, u):
        span = jnp.zeros((spans, BLOCK), jnp.float32)
        for client in range(clients):
            lines = pl.ds(client * spans, spans)
            grad = acc[lines, :] * slope[chunk, lines, :].astype(jnp.float32)
            span = span + grad
            sums[u, pl.ds(spans + client, 1), :] = jnp.sum(grad, axis=0, keepdims=True)
        sums[u, pl.ds(0, spans), :] = span

    for part in range(4):
        weight_copy(part).wait()

    def second_product(g, carry):
        before, table = carry
        chunk0 = lax.rem(y + lax.rem(table, 4), 4) * 4
        for t in range(4):
            u = 4 * g + t
            now, last = (acc_a, acc_b) if t % 2 == 0 else (acc_b, acc_a)
            chunk = chunk0 + t
            previous = before if t == 0 else chunk - 1
            slot = lax.rem(u + STEPS, STEPS + 1)
            reduce_rows(last, previous, slot)
            lines = pl.ds(pl.multiple_of(chunk * BLOCK, BLOCK), BLOCK)
            now[...] = lax.dot_general(low[...], weight[lines, :], (((1,), (1,)), ((), ())), preferred_element_type=jnp.float32)
            if t == 1:

                @pl.when(g == 0)
                def _():
                    core_add(STEPS - 2)
                    core_add(STEPS - 1)
                    do_b(3)
                    do_f(1)

                for group in range(3):

                    @pl.when(g == group + 1)
                    def _(group=group):
                        for k in range(4):
                            sums_low[4 * group + k] = sums[4 * group + k].astype(jnp.bfloat16)
                        y_copy(group).start()

                @pl.when(g == 1)
                def _():
                    do_f(2)
                    do_b2()

                pl.when(g == 2)(lambda: do_f(3))
            elif t == 3:
                pl.when(g == 2)(do_final)
        return chunk0 + 3, lax.div(table, 4)

    final_chunk, _ = lax.fori_loop(0, 4, second_product, (jnp.int32(0), jnp.int32(digits(YORDER))))
    reduce_rows(acc_b, final_chunk, STEPS - 1)

    for group in range(3):
        y_copy(group).wait_recv()
    embed_square = jnp.zeros((1, LANES), jnp.float32)
    for t in range(4):
        total = sums[12 + t]
        for group in range(3):
            total = total + yrecv[group, t].astype(jnp.float32)
        lanes = pl.ds(t * BLOCK, BLOCK)
        rest_own[pl.ds(0, spans), lanes] = total[:spans].astype(jnp.bfloat16)
        mine = total[spans:]
        emb[0, 0, :, lanes] = mine.astype(jnp.bfloat16)
        square = jnp.sum(mine * mine, axis=0, keepdims=True)
        embed_square = embed_square + square[:, :LANES] + square[:, LANES:]
    squares[0, pl.ds(1, 1), :] = embed_square
    over(1, 32, lambda o: scatter_copy(o).start())
    start_all(embed_copies(0))
    over(1, 32, lambda o: scatter_copy(o).wait_recv())
    piece = rest_own[piece_of(z, x, c)].astype(jnp.float32)
    piece = piece + jnp.sum(rest_in[1:].astype(jnp.float32), axis=0)
    rest_all[piece_of(z, x, c)] = piece.astype(jnp.bfloat16)
    squares[0, pl.ds(2, 1), :] = jnp.sum(piece * piece, axis=0, keepdims=True)
    over(1, 32, lambda o: gather_copy(o).start())
    over(1, 16, lambda o: plane_copy(o).start())
    arrive_all(embed_copies(0))
    start_all(embed_copies(1))
    over(1, 16, lambda o: plane_copy(o).wait_recv())
    squares[1] = squares[0] + jnp.sum(squares_zx[1:], axis=0)
    over(1, 8, lambda o: column_copy(o).start())
    over(1, 32, lambda o: gather_copy(o).wait_recv())
    arrive_all(id_copies(1))
    lane = lax.broadcasted_iota(jnp.int32, (1, LANES), 1)
    chip = (z * 4 + x) * 2
    wanted = jnp.where(lane < clients, (chip + c) * clients + lane, jnp.where(lane < 2 * clients, (chip + 1 - c) * clients + lane - clients, -1))
    chosen = (ids[...].reshape(16 * clients, LANES) == wanted).astype(jnp.float32).astype(jnp.bfloat16)
    arrive_all(embed_copies(1))
    table = lax.dot_general(chosen, emb[...].reshape(16 * clients, here), (((0,), (0,)), ((), ())), preferred_element_type=jnp.float32)
    picked[...] = table[clients : 2 * clients].astype(jnp.bfloat16)
    picked_copy().start()
    over(1, 8, lambda o: column_copy(o).wait_recv())
    totals = squares[1] + jnp.sum(squares_y[1:], axis=0)

    def factor(line, number):
        total = jnp.sum(totals[line : line + 1], axis=1, keepdims=True)
        return jnp.minimum(1.0, 1.0 / jnp.sqrt(total / number + EPSILON))

    width = weight.shape[0]
    emit = here * 4
    head_out[...] = head_out[...] * factor(0, width * emit)
    rest = factor(2, spans * width + emit)
    span_out[...] = rest_all[pl.ds(0, spans), :].astype(jnp.float32) * rest
    bias_out[...] = rest_all[pl.ds(spans, 16), :].astype(jnp.float32)[:1] * rest
    embed_factor = factor(1, 32 * clients * width)
    picked_copy().wait_recv()
    embed_out[...] = (table[:clients] + picked_in[...].astype(jnp.float32)) * embed_factor

    over(0, STEPS, lambda s: core_copy(s).wait_send())
    sent = [*a2_copies(), *b2_copies(), picked_copy()]
    for i in range(4):
        sent += [*a_copies(i), *b_copies(i)]
    for group in range(3):
        sent.append(y_copy(group))
    for k in range(2):
        sent += [*id_copies(k), *embed_copies(k)]
    for copy in sent:
        copy.wait_send()
    over(1, 32, lambda o: scatter_copy(o).wait_send())
    over(1, 32, lambda o: gather_copy(o).wait_send())
    over(1, 16, lambda o: plane_copy(o).wait_send())
    over(1, 8, lambda o: column_copy(o).wait_send())


def per_device(pre, delta, head_weight, client_ids):
    rows, width = pre.shape
    here = delta.shape[1]
    clients = client_ids.shape[0]
    bf16, f32 = jnp.bfloat16, jnp.float32
    dma = pltpu.SemaphoreType.DMA
    spans = rows // clients
    anywhere = pl.BlockSpec(memory_space=pl.ANY)
    in_vmem = pl.BlockSpec(memory_space=pltpu.VMEM)
    head, bias, embed, span = pl.pallas_call(
        kernel,
        name="products",
        out_shape=(
            jax.ShapeDtypeStruct((LANES, here), f32),
            jax.ShapeDtypeStruct((1, here), f32),
            jax.ShapeDtypeStruct((clients, here), f32),
            jax.ShapeDtypeStruct((spans, here), f32),
        ),
        in_specs=[anywhere] * 3 + [pl.BlockSpec(memory_space=pltpu.SMEM)],
        out_specs=[in_vmem] * 4,
        scratch_shapes=[
            pltpu.VMEM((3, 256, here), f32),
            pltpu.VMEM((rows, here), bf16),
            pltpu.VMEM((here, rows), bf16),
            pltpu.VMEM((width, here), bf16),
            pltpu.VMEM((4, rows, BLOCK), bf16),
            pltpu.VMEM((rows, BLOCK), bf16),
            pltpu.VMEM((rows, BLOCK), bf16),
            pltpu.VMEM((STEPS + 1, rows, BLOCK), bf16),
            pltpu.VMEM((STEPS, 2, here, LANES), bf16),
            pltpu.VMEM((STEPS, here, LANES), bf16),
            pltpu.VMEM((rows, BLOCK), f32),
            pltpu.VMEM((rows, BLOCK), f32),
            pltpu.VMEM((STEPS + 1, spans + 16, BLOCK), f32),
            pltpu.VMEM((12, spans + 16, BLOCK), bf16),
            pltpu.VMEM((3, 4, spans + 16, BLOCK), bf16),
            pltpu.VMEM((4, 2, here // 2, LANES), bf16),
            pltpu.VMEM((4, 2, here, LANES), bf16),
            pltpu.VMEM((2, here // 2, LANES), bf16),
            pltpu.VMEM((2, here, LANES), bf16),
            pltpu.VMEM((4, 4, clients, LANES), jnp.int32),
            pltpu.VMEM((4, 4, clients, here), bf16),
            pltpu.VMEM((128, here), bf16),
            pltpu.VMEM((32, 32, LANES), bf16),
            pltpu.VMEM((128, here), bf16),
            pltpu.VMEM((clients, here), bf16),
            pltpu.VMEM((clients, here), bf16),
            pltpu.VMEM((2, 8, LANES), f32),
            pltpu.VMEM((16, 8, LANES), f32),
            pltpu.VMEM((8, 8, LANES), f32),
            dma((3,)),
            dma((4,)),
            dma((4, 2)),
            *[dma((STEPS,))] * 2,
            *[dma((4, 2))] * 2,
            *[dma((4, 4))] * 2,
            *[dma((2,))] * 2,
            *[dma((4,))] * 2,
            *[dma((3,))] * 2,
            *[dma((2, 4))] * 4,
            *[dma((32,))] * 4,
            *[dma((1,))] * 2,
            *[dma((16,))] * 2,
            *[dma((8,))] * 2,
        ],
        compiler_params=pltpu.CompilerParams(collective_id=0, has_side_effects=True, vmem_limit_bytes=67_000_000),
    )(pre, delta, head_weight, client_ids)
    return head, bias[0], embed, span


def solution(mesh):
    torus = Mesh(
        mesh.devices.reshape(4, 4, 2, mesh.shape["head"]),
        ("client_0", "client_1", "client_2", "head"),
    )
    return jax.shard_map(
        per_device,
        mesh=torus,
        in_specs=(P(CLIENT, None), P(CLIENT, "head"), P(None, "head"), P(CLIENT)),
        out_specs=(P(CLIENT, "head"), P("head"), P(CLIENT, "head"), P(None, "head")),
        check_vma=False,
    )
```

```python
import jax
import jax.numpy as jnp
from jax import lax
from jax.experimental import pallas as pl
from jax.experimental.pallas import tpu as pltpu
from jax.sharding import Mesh
from jax.sharding import PartitionSpec as P

CLIENT = ("client_0", "client_1", "client_2")
EPSILON = 1e-06
MESH = pl.DeviceIdType.MESH

ORDER = ((2, 2), (2, 1), (2, 3), (2, 0), (1, 2), (3, 2), (0, 2), (1, 1), (3, 1), (0, 1), (1, 3), (3, 3), (0, 3), (1, 0), (3, 0), (0, 0))
STEPS = 16
BLOCK = 256
LANES = 128
YORDER = (2, 1, 3, 0)


def digits(values):
    return sum(v * 4**i for i, v in enumerate(values))


def kernel(
    pre_hbm, delta_hbm, weight_hbm, ids_ref, head_out, rest_out, embed_out, total_out,
    stage, low, low_t, weight, pre_b, hid_a, hid_b, slope, prod, crecv, acc_a, acc_b, sums, span_low, rows_low, span_in, rows_in, own_send, own_in, bias_rows, r_a, r_b, r_a2, r_b2,
    ids, emb, rest_own, rest_in, rest_all, picked, picked_in, squares, squares_zx, squares_y,
    delta_sem, weight_sem, pre_sem, c_send, c_recv, a_send, a_recv, b_send, b_recv, a2_send, a2_recv, b2_send, b2_recv, y_send, y_recv, ys_send, ys_recv, own_sems,
    i_send, i_recv, e_send, e_recv, rs_send, rs_recv, ag_send, ag_recv, p_send, p_recv, zx_send, zx_recv, sy_send, sy_recv,
):
    rows = low.shape[0]
    here = low.shape[1]
    clients = 16
    spans = rows // clients
    half = prod.shape[2] // 2
    z, x, c, y = (lax.axis_index(a) for a in (*CLIENT, "head"))

    def ring(one, offset):
        along_z = one * (1 - c) + (1 - one) * c
        return lax.rem(z + offset * along_z, 4), lax.rem(x + offset * (1 - along_z), 4), c, y

    def client_peer(o):
        return lax.rem(z + lax.div(o, 8), 4), lax.rem(x + lax.rem(lax.div(o, 2), 4), 4), lax.rem(c + lax.rem(o, 2), 2), y

    def plane_peer(o):
        return lax.rem(z + lax.div(o, 4), 4), lax.rem(x + lax.rem(o, 4), 4), c, y

    def column_peer(o):
        return z, x, lax.rem(c + lax.rem(o, 2), 2), lax.rem(y + lax.div(o, 2), 4)

    partner = (z, x, 1 - c, y)
    barrier = pltpu.get_barrier_semaphore()

    def greet(peer, first, last):
        def one(o, carry):
            pl.semaphore_signal(barrier, inc=1, device_id=peer(o), device_id_type=MESH)
            return carry

        lax.fori_loop(first, last, one, 0)

    greet(client_peer, 1, 32)
    greet(column_peer, 2, 8)

    def delta_copy(block):
        slot = block % 3
        return pltpu.make_async_copy(delta_hbm.at[pl.ds(block * 256, 256), :], stage.at[slot], delta_sem.at[slot])

    def chips(dp, dq):
        first = lax.rem(z + dp, 4) * 4 + lax.rem(x + dq, 4)
        second = lax.rem(z + dq, 4) * 4 + lax.rem(x + dp, 4)
        return first, second

    def pre_copies(dp, dq, slot):
        out = []
        for h, chip in enumerate(chips(dp, dq)):
            column = pl.multiple_of((chip * 2 + h) * LANES, LANES)
            out.append(
                pltpu.make_async_copy(
                    pre_hbm.at[:, pl.ds(column, LANES)],
                    pre_b.at[slot, :, pl.ds(h * LANES, LANES)],
                    pre_sem.at[slot, h],
                )
            )
        return out

    def weight_copy(part):
        size = weight.shape[0] // 4
        return pltpu.make_async_copy(weight_hbm.at[pl.ds(part * size, size), :], weight.at[pl.ds(part * size, size), :], weight_sem.at[part])

    def silu_to(slot, hid, at):
        for b in range(rows // 32):
            lines = pl.ds(b * 32, 32)
            v = pre_b[slot, lines, :].astype(jnp.float32)
            gate = 1.0 / (1.0 + jnp.exp(-v))
            value = v * gate
            hid[lines, :] = value.astype(jnp.bfloat16)
            slant = (gate + value * (1.0 - gate)).astype(jnp.bfloat16)
            for h in range(2):
                slope[at[h], lines, pl.ds(h * LANES, LANES)] = slant[:, h * LANES : (h + 1) * LANES]

    def remote(src, dst, send, recv, to):
        return pltpu.make_async_remote_copy(src_ref=src, dst_ref=dst, send_sem=send, recv_sem=recv, device_id=to, device_id_type=MESH)

    lower, upper = pl.ds(0, half), pl.ds(half, half)

    def core_copy(s):
        return remote(prod.at[s, 1 - c], crecv.at[s], c_send.at[s], c_recv.at[s], partner)

    def a_copies(i):
        return (
            remote(prod.at[i, c, lower], r_a.at[i, 0], a_send.at[i, 0], a_recv.at[i, 0], ring(1, 3)),
            remote(prod.at[i, c, upper], r_a.at[i, 1], a_send.at[i, 1], a_recv.at[i, 1], ring(1, 1)),
        )

    def b_copies(i):
        ahead, behind = 4 + 3 * i, 5 + 3 * i

        def one(chunk, part, side, k, to):
            return remote(prod.at[chunk, c, part], r_b.at[i, side, part], b_send.at[i, k], b_recv.at[i, k], to)

        return (
            one(ahead, lower, 0, 0, ring(1, 1)),
            one(behind, upper, 1, 1, ring(1, 3)),
            one(ahead, upper, 0, 2, ring(1, 1)),
            one(behind, lower, 1, 3, ring(1, 3)),
        )

    def a2_copies():
        chunk = 6
        return (
            remote(prod.at[chunk, c, lower], r_a2.at[0], a2_send.at[0], a2_recv.at[0], ring(0, 3)),
            remote(prod.at[chunk, c, upper], r_a2.at[1], a2_send.at[1], a2_recv.at[1], ring(0, 1)),
        )

    def b2_copies():
        def one(chunk, part, side, k, to):
            return remote(prod.at[chunk, c, part], r_b2.at[side, part], b2_send.at[k], b2_recv.at[k], to)

        return (
            one(9, lower, 0, 0, ring(0, 1)),
            one(12, upper, 1, 1, ring(0, 3)),
            one(9, upper, 0, 2, ring(0, 1)),
            one(12, lower, 1, 3, ring(0, 3)),
        )

    def y_target(group):
        return lax.rem(y + YORDER[group], 4)

    def y_rows(group):
        return remote(rows_low.at[group], rows_in.at[group], y_send.at[group], y_recv.at[group], (z, x, c, y_target(group)))

    def y_spans(group, side):
        mine = span_low.at[pl.ds(4 * group + 2 * side, 2)]
        return remote(mine, span_in.at[group, c], ys_send.at[group, side], ys_recv.at[group, c], (z, x, side, y_target(group)))

    def y_arrival(group, core):
        mine = span_low.at[pl.ds(4 * group, 2)]
        return remote(mine, span_in.at[group, core], ys_send.at[group, core], ys_recv.at[group, core], (z, x, core, y_target(group)))

    def own_copy():
        return remote(own_send, own_in, own_sems.at[0], own_sems.at[1], partner)

    def send_spans(group, side):
        for k in range(2):
            chunk = 4 * group + 2 * side + k
            span_low[chunk] = sums[chunk, pl.ds(0, spans), :].astype(jnp.bfloat16)
        y_spans(group, side).start()

    def id_copies(stage_):
        if stage_ == 0:
            return [remote(ids.at[0, 0], ids.at[0, o], i_send.at[0, o], i_recv.at[0, o], ring(1, o)) for o in (2, 1, 3)]
        return [remote(ids.at[0], ids.at[o], i_send.at[1, o], i_recv.at[1, o], ring(0, o)) for o in (2, 1, 3)]

    def embed_copies(stage_):
        if stage_ == 0:
            return [remote(emb.at[0, 0], emb.at[0, o], e_send.at[0, o], e_recv.at[0, o], ring(1, o)) for o in (2, 1, 3)]
        return [remote(emb.at[0], emb.at[o], e_send.at[1, o], e_recv.at[1, o], ring(0, o)) for o in (2, 1, 3)]

    def piece_of(line, tile):
        return pl.ds(pl.multiple_of(line * 32, 32), 32), pl.ds(pl.multiple_of(tile * LANES, LANES), LANES)

    def scatter_copy(o):
        to = plane_peer(o)
        return remote(rest_own.at[piece_of(to[0], to[1])], rest_in.at[o], rs_send.at[o], rs_recv.at[o], to)

    def gather_copy(o):
        mine = piece_of(z, c * 4 + x)
        return remote(rest_all.at[mine], rest_all.at[mine], ag_send.at[o], ag_recv.at[o], client_peer(o))

    def picked_copy():
        return remote(picked, picked_in, p_send.at[0], p_recv.at[0], partner)

    def plane_copy(o):
        return remote(squares.at[0], squares_zx.at[o], zx_send.at[o], zx_recv.at[o], plane_peer(o))

    def column_copy(o):
        return remote(squares.at[1], squares_y.at[o], sy_send.at[o], sy_recv.at[o], column_peer(o))

    def over(first, last, what):
        def one(o, carry):
            what(o)
            return carry

        lax.fori_loop(first, last, one, 0)

    def start_all(copies):
        for copy in copies:
            copy.start()

    def arrive_all(copies):
        for copy in copies:
            copy.wait_recv()

    def core_add(s):
        core_copy(s).wait_recv()
        prod[s, c] = prod[s, c] + crecv[s]

    def do_b(i):
        first, second, third, fourth = b_copies(i)
        first.start()
        second.start()
        from_plus, from_minus = a_copies(i)
        ahead, behind = 4 + 3 * i, 5 + 3 * i
        from_minus.wait_recv()
        prod[ahead, c, upper] = prod[ahead, c, upper] + r_a[i, 1]
        from_plus.wait_recv()
        prod[behind, c, lower] = prod[behind, c, lower] + r_a[i, 0]
        third.start()
        fourth.start()

    def three(a, b, d):
        return a.astype(jnp.float32) + b.astype(jnp.float32) + d.astype(jnp.float32)

    def do_f(i):
        arrive_all(b_copies(i))
        chunk = 6 + 3 * i
        prod[chunk, c] = three(prod[chunk, c], r_b[i, 0], r_b[i, 1]).astype(jnp.bfloat16)

    def do_b2():
        first, second, third, fourth = b2_copies()
        first.start()
        second.start()
        from_plus, from_minus = a2_copies()
        from_minus.wait_recv()
        prod[9, c, upper] = prod[9, c, upper] + r_a2[1]
        from_plus.wait_recv()
        prod[12, c, lower] = prod[12, c, lower] + r_a2[0]
        third.start()
        fourth.start()

    def do_final():
        arrive_all(b2_copies())
        whole = three(prod[15, c], r_b2[0], r_b2[1])
        squares[0, pl.ds(0, 1), :] = jnp.sum(whole * whole, axis=0, keepdims=True)
        head_out[...] = whole.T

    start_all(pre_copies(*ORDER[0], 0))
    for block in range(3):
        delta_copy(block).start()
    for s in range(1, 4):
        start_all(pre_copies(*ORDER[s], s))
    for client in range(clients):
        ids[0, 0, pl.ds(client, 1), :] = jnp.full((1, LANES), ids_ref[client], jnp.int32)
    squares[...] = jnp.zeros(squares.shape, jnp.float32)
    rest_own[pl.ds(96, 32), :] = jnp.zeros((32, here // 2), jnp.bfloat16)
    for copy in pre_copies(*ORDER[0], 0):
        copy.wait()
    silu_to(0, hid_a, chips(*ORDER[0]))
    start_all(pre_copies(*ORDER[4], 0))
    bias = jnp.zeros((1, here), jnp.float32)
    for block in range(rows // 256):
        delta_copy(block).wait()
        lines = pl.ds(block * 256, 256)
        values = stage[block % 3]
        bias = bias + jnp.sum(values, axis=0, keepdims=True)
        rounded = values.astype(jnp.bfloat16)
        low[lines, :] = rounded
        low_t[:, lines] = rounded.T
        if block + 3 < rows // 256:
            delta_copy(block + 3).start()
    first_line = lax.broadcasted_iota(jnp.int32, (16, here), 0) == 0
    bias_rows[...] = jnp.where(first_line, jnp.broadcast_to(bias, (16, here)), 0.0)
    for part in range(4):
        weight_copy(part).start()

    next_p, next_q = digits([o[0] for o in ORDER[1:]]), digits([o[1] for o in ORDER[1:]])
    load_p, load_q = digits([o[0] for o in ORDER[5:]]), digits([o[1] for o in ORDER[5:]])

    def first_product(i, carry):
        np_, nq_, lp_, lq_ = carry
        offsets, slots = [], []
        for k in range(2):
            offsets.append((lax.rem(np_, 4), lax.rem(nq_, 4)))
            slots.append(lax.rem(2 * i + k + 1, 4))
            np_, nq_ = lax.div(np_, 4), lax.div(nq_, 4)

        def arrived(k):
            for copy in pre_copies(*offsets[k], slots[k]):
                copy.wait()

        arrived(0)
        pl.when(i < STEPS // 2 - 1)(lambda: arrived(1))
        last = lax.div(i, STEPS // 2 - 1)
        for k, (now, later) in enumerate(((hid_a, hid_b), (hid_b, hid_a))):
            s = 2 * i + k
            spare = last if k == 1 else 0
            at = [chip * (1 - spare) + STEPS * spare for chip in chips(*offsets[k])]
            silu_to(slots[k], later, at)
            product = jnp.dot(low_t[...], now[...], preferred_element_type=jnp.float32).astype(jnp.bfloat16)
            for h in range(2):
                prod[s, h] = product[:, h * LANES : (h + 1) * LANES]

        @pl.when(i == 0)
        def _():
            pl.semaphore_wait(barrier, 37)
            start_all(id_copies(0))

        core_copy(2 * i).start()
        core_copy(2 * i + 1).start()
        for k in range(2):

            @pl.when(2 * i + k + 5 < STEPS)
            def _(k=k, lp_=lp_, lq_=lq_):
                start_all(pre_copies(lax.rem(lp_, 4), lax.rem(lq_, 4), slots[k]))

            lp_, lq_ = lax.div(lp_, 4), lax.div(lq_, 4)

        @pl.when(i == 1)
        def _():
            arrive_all(id_copies(0))
            start_all(id_copies(1))

        @pl.when(i >= 1)
        def _():
            core_add(2 * i - 2)
            core_add(2 * i - 1)

        @pl.when(i == 1)
        def _():
            start_all(a_copies(0))
            start_all(a_copies(1))

        @pl.when(i == 2)
        def _():
            start_all(a_copies(2))
            start_all(a_copies(3))

        pl.when(i == 3)(lambda: do_b(0))
        pl.when(i == 5)(lambda: do_b(1))

        @pl.when(i == 6)
        def _():
            do_b(2)
            do_f(0)
            start_all(a2_copies())

        return np_, nq_, lp_, lq_

    lax.fori_loop(0, STEPS // 2, first_product, tuple(jnp.int32(t) for t in (next_p, next_q, load_p, load_q)))

    def reduce_rows(acc, chunk, u):
        span = jnp.zeros((spans, BLOCK), jnp.float32)
        for client in range(clients):
            lines = pl.ds(client * spans, spans)
            grad = acc[lines, :] * slope[chunk, lines, :].astype(jnp.float32)
            span = span + grad
            sums[u, pl.ds(spans + client, 1), :] = jnp.sum(grad, axis=0, keepdims=True)
        sums[u, pl.ds(0, spans), :] = span

    for part in range(4):
        weight_copy(part).wait()

    def second_product(g, carry):
        before, table = carry
        chunk0 = lax.rem(y + lax.rem(table, 4), 4) * 4
        for t in range(4):
            u = 4 * g + t
            now, last = (acc_a, acc_b) if t % 2 == 0 else (acc_b, acc_a)
            chunk = chunk0 + t
            previous = before if t == 0 else chunk - 1
            slot = lax.rem(u + STEPS, STEPS + 1)
            reduce_rows(last, previous, slot)
            lines = pl.ds(pl.multiple_of(chunk * BLOCK, BLOCK), BLOCK)
            now[...] = lax.dot_general(low[...], weight[lines, :], (((1,), (1,)), ((), ())), preferred_element_type=jnp.float32)
            if t == 1:

                @pl.when(g == 0)
                def _():
                    core_add(STEPS - 2)
                    core_add(STEPS - 1)
                    do_b(3)
                    do_f(1)

                for group in range(3):

                    @pl.when(g == group + 1)
                    def _(group=group):
                        send_spans(group, 1)
                        for k in range(4):
                            rows_low[group, k] = sums[4 * group + k, pl.ds(spans, clients), :].astype(jnp.bfloat16)
                        y_rows(group).start()

                @pl.when(g == 1)
                def _():
                    do_f(2)
                    do_b2()

                pl.when(g == 2)(lambda: do_f(3))
            elif t == 3:
                for group in range(3):
                    pl.when(g == group)(lambda group=group: send_spans(group, 0))
                pl.when(g == 2)(do_final)
        return chunk0 + 3, lax.div(table, 4)

    final_chunk, _ = lax.fori_loop(0, 4, second_product, (jnp.int32(0), jnp.int32(digits(YORDER))))
    reduce_rows(acc_b, final_chunk, STEPS - 1)

    half_here = here // 2
    for t in range(2):
        lanes = pl.ds(pl.multiple_of((1 - c) * half_here + t * BLOCK, BLOCK), BLOCK)
        own_send[t, pl.ds(0, spans), :] = sums[12 + 2 * (1 - c) + t, pl.ds(0, spans), :].astype(jnp.bfloat16)
        own_send[t, pl.ds(spans, 16), :] = bias_rows[:, lanes].astype(jnp.bfloat16)
    own_copy().start()
    for group in range(3):
        y_rows(group).wait_recv()
        for core in range(2):
            y_arrival(group, core).wait_recv()
    embed_square = jnp.zeros((1, LANES), jnp.float32)
    for t in range(4):
        mine = sums[12 + t, pl.ds(spans, clients), :]
        for group in range(3):
            mine = mine + rows_in[group, t].astype(jnp.float32)
        emb[0, 0, :, pl.ds(t * BLOCK, BLOCK)] = mine.astype(jnp.bfloat16)
        square = jnp.sum(mine * mine, axis=0, keepdims=True)
        embed_square = embed_square + square[:, :LANES] + square[:, LANES:]
    own_copy().wait_recv()
    for t in range(2):
        total = sums[12 + 2 * c + t, pl.ds(0, spans), :] + own_in[t, pl.ds(0, spans), :].astype(jnp.float32)
        for group in range(3):
            for core in range(2):
                total = total + span_in[group, core, t].astype(jnp.float32)
        lanes = pl.ds(t * BLOCK, BLOCK)
        rest_own[pl.ds(0, spans), lanes] = total.astype(jnp.bfloat16)
        mine = bias_rows[:, pl.ds(pl.multiple_of(c * half_here + t * BLOCK, BLOCK), BLOCK)]
        rest_own[pl.ds(spans, 16), lanes] = (mine + own_in[t, pl.ds(spans, 16), :].astype(jnp.float32)).astype(jnp.bfloat16)
    squares[0, pl.ds(1, 1), :] = embed_square
    over(1, 16, lambda o: scatter_copy(o).start())
    start_all(embed_copies(0))
    over(1, 16, lambda o: scatter_copy(o).wait_recv())
    piece = rest_own[piece_of(z, x)].astype(jnp.float32)
    piece = piece + jnp.sum(rest_in[1:].astype(jnp.float32), axis=0)
    rest_all[piece_of(z, c * 4 + x)] = piece.astype(jnp.bfloat16)
    squares[0, pl.ds(2, 1), :] = jnp.sum(piece * piece, axis=0, keepdims=True)
    over(1, 32, lambda o: gather_copy(o).start())
    over(1, 16, lambda o: plane_copy(o).start())
    arrive_all(embed_copies(0))
    start_all(embed_copies(1))
    over(1, 16, lambda o: plane_copy(o).wait_recv())
    squares[1] = squares[0] + jnp.sum(squares_zx[1:], axis=0)
    over(1, 8, lambda o: column_copy(o).start())
    over(1, 32, lambda o: gather_copy(o).wait_recv())
    arrive_all(id_copies(1))
    lane = lax.broadcasted_iota(jnp.int32, (1, LANES), 1)
    chip = (z * 4 + x) * 2
    wanted = jnp.where(lane < clients, (chip + c) * clients + lane, jnp.where(lane < 2 * clients, (chip + 1 - c) * clients + lane - clients, -1))
    chosen = (ids[...].reshape(16 * clients, LANES) == wanted).astype(jnp.float32).astype(jnp.bfloat16)
    arrive_all(embed_copies(1))
    table = lax.dot_general(chosen, emb[...].reshape(16 * clients, here), (((0,), (0,)), ((), ())), preferred_element_type=jnp.float32)
    picked[...] = table[clients : 2 * clients].astype(jnp.bfloat16)
    picked_copy().start()
    over(1, 8, lambda o: column_copy(o).wait_recv())
    total_out[...] = squares[1] + jnp.sum(squares_y[1:], axis=0)
    rest_out[...] = rest_all[pl.ds(0, spans + 16), :]
    picked_copy().wait_recv()
    embed_out[...] = table[:clients] + picked_in[...].astype(jnp.float32)

    over(0, STEPS, lambda s: core_copy(s).wait_send())
    sent = [*a2_copies(), *b2_copies(), picked_copy(), own_copy()]
    for i in range(4):
        sent += [*a_copies(i), *b_copies(i)]
    for group in range(3):
        sent += [y_rows(group), y_spans(group, 0), y_spans(group, 1)]
    for k in range(2):
        sent += [*id_copies(k), *embed_copies(k)]
    for copy in sent:
        copy.wait_send()
    over(1, 16, lambda o: scatter_copy(o).wait_send())
    over(1, 32, lambda o: gather_copy(o).wait_send())
    over(1, 16, lambda o: plane_copy(o).wait_send())
    over(1, 8, lambda o: column_copy(o).wait_send())


def scale(head, rest, embed, total, head_out, bias_out, embed_out, span_out):
    spans, here = span_out.shape
    width, emit = here * 4, here * 4

    def factor(line, number):
        whole = jnp.sum(total[pl.ds(line, 1), :], axis=1, keepdims=True)
        return jnp.minimum(1.0, 1.0 / jnp.sqrt(whole / number + EPSILON))

    head_out[...] = head[...] * factor(0, width * emit)
    embed_out[...] = embed[...] * factor(1, 32 * embed.shape[0] * width)
    small = factor(2, spans * width + emit)
    span_out[...] = rest[pl.ds(0, spans), :].astype(jnp.float32) * small
    bias_out[...] = rest[pl.ds(spans, 16), :].astype(jnp.float32)[:1] * small


def per_device(pre, delta, head_weight, client_ids):
    rows, width = pre.shape
    here = delta.shape[1]
    clients = client_ids.shape[0]
    bf16, f32 = jnp.bfloat16, jnp.float32
    dma = pltpu.SemaphoreType.DMA
    spans = rows // clients
    anywhere = pl.BlockSpec(memory_space=pl.ANY)
    in_vmem = pl.BlockSpec(memory_space=pltpu.VMEM)
    head, rest, embed, total = pl.pallas_call(
        kernel,
        name="products",
        out_shape=(
            jax.ShapeDtypeStruct((LANES, here), f32),
            jax.ShapeDtypeStruct((spans + 16, here), bf16),
            jax.ShapeDtypeStruct((clients, here), f32),
            jax.ShapeDtypeStruct((8, LANES), f32),
        ),
        in_specs=[anywhere] * 3 + [pl.BlockSpec(memory_space=pltpu.SMEM)],
        out_specs=[in_vmem] * 4,
        scratch_shapes=[
            pltpu.VMEM((3, 256, here), f32),
            pltpu.VMEM((rows, here), bf16),
            pltpu.VMEM((here, rows), bf16),
            pltpu.VMEM((width, here), bf16),
            pltpu.VMEM((4, rows, BLOCK), bf16),
            pltpu.VMEM((rows, BLOCK), bf16),
            pltpu.VMEM((rows, BLOCK), bf16),
            pltpu.VMEM((STEPS + 1, rows, BLOCK), bf16),
            pltpu.VMEM((STEPS, 2, here, LANES), bf16),
            pltpu.VMEM((STEPS, here, LANES), bf16),
            pltpu.VMEM((rows, BLOCK), f32),
            pltpu.VMEM((rows, BLOCK), f32),
            pltpu.VMEM((STEPS + 1, spans + 16, BLOCK), f32),
            pltpu.VMEM((12, spans, BLOCK), bf16),
            pltpu.VMEM((3, 4, clients, BLOCK), bf16),
            pltpu.VMEM((3, 2, 2, spans, BLOCK), bf16),
            pltpu.VMEM((3, 4, clients, BLOCK), bf16),
            pltpu.VMEM((2, spans + 16, BLOCK), bf16),
            pltpu.VMEM((2, spans + 16, BLOCK), bf16),
            pltpu.VMEM((16, here), f32),
            pltpu.VMEM((4, 2, here // 2, LANES), bf16),
            pltpu.VMEM((4, 2, here, LANES), bf16),
            pltpu.VMEM((2, here // 2, LANES), bf16),
            pltpu.VMEM((2, here, LANES), bf16),
            pltpu.VMEM((4, 4, clients, LANES), jnp.int32),
            pltpu.VMEM((4, 4, clients, here), bf16),
            pltpu.VMEM((128, here // 2), bf16),
            pltpu.VMEM((16, 32, LANES), bf16),
            pltpu.VMEM((128, here), bf16),
            pltpu.VMEM((clients, here), bf16),
            pltpu.VMEM((clients, here), bf16),
            pltpu.VMEM((2, 8, LANES), f32),
            pltpu.VMEM((16, 8, LANES), f32),
            pltpu.VMEM((8, 8, LANES), f32),
            dma((3,)),
            dma((4,)),
            dma((4, 2)),
            *[dma((STEPS,))] * 2,
            *[dma((4, 2))] * 2,
            *[dma((4, 4))] * 2,
            *[dma((2,))] * 2,
            *[dma((4,))] * 2,
            *[dma((3,))] * 2,
            *[dma((3, 2))] * 2,
            dma((2,)),
            *[dma((2, 4))] * 4,
            *[dma((16,))] * 2,
            *[dma((32,))] * 2,
            *[dma((1,))] * 2,
            *[dma((16,))] * 2,
            *[dma((8,))] * 2,
        ],
        compiler_params=pltpu.CompilerParams(collective_id=0, has_side_effects=True, vmem_limit_bytes=67_000_000),
    )(pre, delta, head_weight, client_ids)
    head, bias, embed, span = pl.pallas_call(
        scale,
        name="scale",
        out_shape=(
            jax.ShapeDtypeStruct((LANES, here), f32),
            jax.ShapeDtypeStruct((1, here), f32),
            jax.ShapeDtypeStruct((clients, here), f32),
            jax.ShapeDtypeStruct((spans, here), f32),
        ),
        in_specs=[in_vmem] * 4,
        out_specs=[in_vmem] * 4,
    )(head, rest, embed, total)
    return head, bias[0], embed, span


def solution(mesh):
    torus = Mesh(
        mesh.devices.reshape(4, 4, 2, mesh.shape["head"]),
        ("client_0", "client_1", "client_2", "head"),
    )
    return jax.shard_map(
        per_device,
        mesh=torus,
        in_specs=(P(CLIENT, None), P(CLIENT, "head"), P(None, "head"), P(CLIENT)),
        out_specs=(P(CLIENT, "head"), P("head"), P(CLIENT, "head"), P(None, "head")),
        check_vma=False,
    )
```

```python
import jax
import jax.numpy as jnp
from jax import lax
from jax.experimental import pallas as pl
from jax.experimental.pallas import tpu as pltpu
from jax.sharding import Mesh
from jax.sharding import PartitionSpec as P

CLIENT = ("client_0", "client_1", "client_2")
EPSILON = 1e-06
MESH = pl.DeviceIdType.MESH

ORDER = ((2, 2), (2, 1), (2, 3), (2, 0), (1, 2), (3, 2), (0, 2), (1, 1), (3, 1), (0, 1), (1, 3), (3, 3), (0, 3), (1, 0), (3, 0), (0, 0))
STEPS = 16
BLOCK = 256
LANES = 128
YORDER = (2, 1, 3, 0)


def digits(values):
    return sum(v * 4**i for i, v in enumerate(values))


def kernel(
    pre_hbm, delta_hbm, weight_hbm, ids_ref, head_out, rest_out, embed_out, total_out,
    stage, low, low_t, weight, pre_b, hid_a, hid_b, slope_a, slope_b, prod, crecv, acc_a, acc_b, sums, span_low, rows_low, span_in, rows_in, own_send, own_in, bias_rows, r_a, r_b, r_a2, r_b2,
    ids, emb, rest_own, rest_in, rest_all, picked, picked_in, squares, squares_zx, squares_y,
    delta_sem, weight_sem, pre_sem, c_send, c_recv, a_send, a_recv, b_send, b_recv, a2_send, a2_recv, b2_send, b2_recv, y_send, y_recv, ys_send, ys_recv, own_sems,
    i_send, i_recv, e_send, e_recv, rs_send, rs_recv, ag_send, ag_recv, p_send, p_recv, zx_send, zx_recv, sy_send, sy_recv,
):
    rows = low.shape[0]
    here = low.shape[1]
    clients = 16
    spans = rows // clients
    half = prod.shape[2] // 2
    z, x, c, y = (lax.axis_index(a) for a in (*CLIENT, "head"))

    def ring(one, offset):
        along_z = one * (1 - c) + (1 - one) * c
        return lax.rem(z + offset * along_z, 4), lax.rem(x + offset * (1 - along_z), 4), c, y

    def client_peer(o):
        return lax.rem(z + lax.div(o, 8), 4), lax.rem(x + lax.rem(lax.div(o, 2), 4), 4), lax.rem(c + lax.rem(o, 2), 2), y

    def plane_peer(o):
        return lax.rem(z + lax.div(o, 4), 4), lax.rem(x + lax.rem(o, 4), 4), c, y

    def column_peer(o):
        return z, x, lax.rem(c + lax.rem(o, 2), 2), lax.rem(y + lax.div(o, 2), 4)

    partner = (z, x, 1 - c, y)
    barrier = pltpu.get_barrier_semaphore()

    def greet(peer, first, last):
        def one(o, carry):
            pl.semaphore_signal(barrier, inc=1, device_id=peer(o), device_id_type=MESH)
            return carry

        lax.fori_loop(first, last, one, 0)

    greet(client_peer, 1, 32)
    greet(column_peer, 2, 8)

    def delta_copy(block):
        slot = block % 3
        return pltpu.make_async_copy(delta_hbm.at[pl.ds(block * 256, 256), :], stage.at[slot], delta_sem.at[slot])

    def chips(dp, dq):
        first = lax.rem(z + dp, 4) * 4 + lax.rem(x + dq, 4)
        second = lax.rem(z + dq, 4) * 4 + lax.rem(x + dp, 4)
        return first, second

    def pre_copies(dp, dq, slot):
        out = []
        for h, chip in enumerate(chips(dp, dq)):
            column = pl.multiple_of((chip * 2 + h) * LANES, LANES)
            out.append(
                pltpu.make_async_copy(
                    pre_hbm.at[:, pl.ds(column, LANES)],
                    pre_b.at[slot, :, pl.ds(h * LANES, LANES)],
                    pre_sem.at[slot, h],
                )
            )
        return out

    def weight_copy(part):
        size = weight.shape[0] // 4
        return pltpu.make_async_copy(weight_hbm.at[pl.ds(part * size, size), :], weight.at[pl.ds(part * size, size), :], weight_sem.at[part])

    def silu_to(slot, hid, at):
        for b in range(rows // 32):
            lines = pl.ds(b * 32, 32)
            v = pre_b[slot, lines, :].astype(jnp.float32)
            gate = 1.0 / (1.0 + jnp.exp(-v))
            value = v * gate
            hid[lines, :] = value.astype(jnp.bfloat16)
            slant = (gate + value * (1.0 - gate)).astype(jnp.bfloat16)
            slope_a[at[0], lines, :] = slant[:, :LANES]
            slope_b[at[1], lines, :] = slant[:, LANES:]

    def remote(src, dst, send, recv, to):
        return pltpu.make_async_remote_copy(src_ref=src, dst_ref=dst, send_sem=send, recv_sem=recv, device_id=to, device_id_type=MESH)

    lower, upper = pl.ds(0, half), pl.ds(half, half)

    def core_copy(s):
        return remote(prod.at[s, 1 - c], crecv.at[s], c_send.at[s], c_recv.at[s], partner)

    def a_copies(i):
        return (
            remote(prod.at[i, c, lower], r_a.at[i, 0], a_send.at[i, 0], a_recv.at[i, 0], ring(1, 3)),
            remote(prod.at[i, c, upper], r_a.at[i, 1], a_send.at[i, 1], a_recv.at[i, 1], ring(1, 1)),
        )

    def b_copies(i):
        ahead, behind = 4 + 3 * i, 5 + 3 * i

        def one(chunk, part, side, k, to):
            return remote(prod.at[chunk, c, part], r_b.at[i, side, part], b_send.at[i, k], b_recv.at[i, k], to)

        return (
            one(ahead, lower, 0, 0, ring(1, 1)),
            one(behind, upper, 1, 1, ring(1, 3)),
            one(ahead, upper, 0, 2, ring(1, 1)),
            one(behind, lower, 1, 3, ring(1, 3)),
        )

    def a2_copies():
        chunk = 6
        return (
            remote(prod.at[chunk, c, lower], r_a2.at[0], a2_send.at[0], a2_recv.at[0], ring(0, 3)),
            remote(prod.at[chunk, c, upper], r_a2.at[1], a2_send.at[1], a2_recv.at[1], ring(0, 1)),
        )

    def b2_copies():
        def one(chunk, part, side, k, to):
            return remote(prod.at[chunk, c, part], r_b2.at[side, part], b2_send.at[k], b2_recv.at[k], to)

        return (
            one(9, lower, 0, 0, ring(0, 1)),
            one(12, upper, 1, 1, ring(0, 3)),
            one(9, upper, 0, 2, ring(0, 1)),
            one(12, lower, 1, 3, ring(0, 3)),
        )

    def y_target(group):
        return lax.rem(y + YORDER[group], 4)

    def y_rows(group):
        return remote(rows_low.at[group], rows_in.at[group], y_send.at[group], y_recv.at[group], (z, x, c, y_target(group)))

    def y_spans(group, side):
        mine = span_low.at[pl.ds(4 * group + 2 * side, 2)]
        return remote(mine, span_in.at[group, c], ys_send.at[group, side], ys_recv.at[group, c], (z, x, side, y_target(group)))

    def y_arrival(group, core):
        mine = span_low.at[pl.ds(4 * group, 2)]
        return remote(mine, span_in.at[group, core], ys_send.at[group, core], ys_recv.at[group, core], (z, x, core, y_target(group)))

    def own_copy():
        return remote(own_send, own_in, own_sems.at[0], own_sems.at[1], partner)

    def send_spans(group, side):
        for k in range(2):
            chunk = 4 * group + 2 * side + k
            span_low[chunk] = sums[chunk, pl.ds(0, spans), :].astype(jnp.bfloat16)
        y_spans(group, side).start()

    def id_copies(stage_):
        if stage_ == 0:
            return [remote(ids.at[0, 0], ids.at[0, o], i_send.at[0, o], i_recv.at[0, o], ring(1, o)) for o in (2, 1, 3)]
        return [remote(ids.at[0], ids.at[o], i_send.at[1, o], i_recv.at[1, o], ring(0, o)) for o in (2, 1, 3)]

    def embed_copies(stage_):
        if stage_ == 0:
            return [remote(emb.at[0, 0], emb.at[0, o], e_send.at[0, o], e_recv.at[0, o], ring(1, o)) for o in (2, 1, 3)]
        return [remote(emb.at[0], emb.at[o], e_send.at[1, o], e_recv.at[1, o], ring(0, o)) for o in (2, 1, 3)]

    def piece_of(line, tile):
        return pl.ds(pl.multiple_of(line * 32, 32), 32), pl.ds(pl.multiple_of(tile * LANES, LANES), LANES)

    def scatter_copy(o):
        to = plane_peer(o)
        return remote(rest_own.at[piece_of(to[0], to[1])], rest_in.at[o], rs_send.at[o], rs_recv.at[o], to)

    def gather_copy(o):
        mine = piece_of(z, c * 4 + x)
        return remote(rest_all.at[mine], rest_all.at[mine], ag_send.at[o], ag_recv.at[o], client_peer(o))

    def picked_copy():
        return remote(picked, picked_in, p_send.at[0], p_recv.at[0], partner)

    def plane_copy(o):
        return remote(squares.at[0], squares_zx.at[o], zx_send.at[o], zx_recv.at[o], plane_peer(o))

    def column_copy(o):
        return remote(squares.at[1], squares_y.at[o], sy_send.at[o], sy_recv.at[o], column_peer(o))

    def over(first, last, what):
        def one(o, carry):
            what(o)
            return carry

        lax.fori_loop(first, last, one, 0)

    def start_all(copies):
        for copy in copies:
            copy.start()

    def arrive_all(copies):
        for copy in copies:
            copy.wait_recv()

    def core_add(s):
        core_copy(s).wait_recv()
        prod[s, c] = prod[s, c] + crecv[s]

    def do_b(i):
        first, second, third, fourth = b_copies(i)
        first.start()
        second.start()
        from_plus, from_minus = a_copies(i)
        ahead, behind = 4 + 3 * i, 5 + 3 * i
        from_minus.wait_recv()
        prod[ahead, c, upper] = prod[ahead, c, upper] + r_a[i, 1]
        from_plus.wait_recv()
        prod[behind, c, lower] = prod[behind, c, lower] + r_a[i, 0]
        third.start()
        fourth.start()

    def three(a, b, d):
        return a.astype(jnp.float32) + b.astype(jnp.float32) + d.astype(jnp.float32)

    def do_f(i):
        arrive_all(b_copies(i))
        chunk = 6 + 3 * i
        prod[chunk, c] = three(prod[chunk, c], r_b[i, 0], r_b[i, 1]).astype(jnp.bfloat16)

    def do_b2():
        first, second, third, fourth = b2_copies()
        first.start()
        second.start()
        from_plus, from_minus = a2_copies()
        from_minus.wait_recv()
        prod[9, c, upper] = prod[9, c, upper] + r_a2[1]
        from_plus.wait_recv()
        prod[12, c, lower] = prod[12, c, lower] + r_a2[0]
        third.start()
        fourth.start()

    def do_final():
        arrive_all(b2_copies())
        whole = three(prod[15, c], r_b2[0], r_b2[1])
        squares[0, pl.ds(0, 1), :] = jnp.sum(whole * whole, axis=0, keepdims=True)
        head_out[...] = whole.T

    start_all(pre_copies(*ORDER[0], 0))
    for block in range(3):
        delta_copy(block).start()
    for s in range(1, 4):
        start_all(pre_copies(*ORDER[s], s))
    for client in range(clients):
        ids[0, 0, pl.ds(client, 1), :] = jnp.full((1, LANES), ids_ref[client], jnp.int32)
    squares[...] = jnp.zeros(squares.shape, jnp.float32)
    rest_own[pl.ds(96, 32), :] = jnp.zeros((32, here // 2), jnp.bfloat16)
    for copy in pre_copies(*ORDER[0], 0):
        copy.wait()
    silu_to(0, hid_a, chips(*ORDER[0]))
    start_all(pre_copies(*ORDER[4], 0))
    bias = jnp.zeros((1, here), jnp.float32)
    for block in range(rows // 256):
        delta_copy(block).wait()
        lines = pl.ds(block * 256, 256)
        values = stage[block % 3]
        bias = bias + jnp.sum(values, axis=0, keepdims=True)
        rounded = values.astype(jnp.bfloat16)
        low[lines, :] = rounded
        low_t[:, lines] = rounded.T
        if block + 3 < rows // 256:
            delta_copy(block + 3).start()
    first_line = lax.broadcasted_iota(jnp.int32, (16, here), 0) == 0
    bias_rows[...] = jnp.where(first_line, jnp.broadcast_to(bias, (16, here)), 0.0)
    for part in range(4):
        weight_copy(part).start()

    next_p, next_q = digits([o[0] for o in ORDER[1:]]), digits([o[1] for o in ORDER[1:]])
    load_p, load_q = digits([o[0] for o in ORDER[5:]]), digits([o[1] for o in ORDER[5:]])

    def first_product(i, carry):
        np_, nq_, lp_, lq_ = carry
        offsets, slots = [], []
        for k in range(2):
            offsets.append((lax.rem(np_, 4), lax.rem(nq_, 4)))
            slots.append(lax.rem(2 * i + k + 1, 4))
            np_, nq_ = lax.div(np_, 4), lax.div(nq_, 4)

        def arrived(k):
            for copy in pre_copies(*offsets[k], slots[k]):
                copy.wait()

        arrived(0)
        pl.when(i < STEPS // 2 - 1)(lambda: arrived(1))
        last = lax.div(i, STEPS // 2 - 1)
        for k, (now, later) in enumerate(((hid_a, hid_b), (hid_b, hid_a))):
            s = 2 * i + k
            spare = last if k == 1 else 0
            at = [chip * (1 - spare) + STEPS * spare for chip in chips(*offsets[k])]
            silu_to(slots[k], later, at)
            product = jnp.dot(low_t[...], now[...], preferred_element_type=jnp.float32).astype(jnp.bfloat16)
            for h in range(2):
                prod[s, h] = product[:, h * LANES : (h + 1) * LANES]

        @pl.when(i == 0)
        def _():
            pl.semaphore_wait(barrier, 37)
            start_all(id_copies(0))

        core_copy(2 * i).start()
        core_copy(2 * i + 1).start()
        for k in range(2):

            @pl.when(2 * i + k + 5 < STEPS)
            def _(k=k, lp_=lp_, lq_=lq_):
                start_all(pre_copies(lax.rem(lp_, 4), lax.rem(lq_, 4), slots[k]))

            lp_, lq_ = lax.div(lp_, 4), lax.div(lq_, 4)

        @pl.when(i == 1)
        def _():
            arrive_all(id_copies(0))
            start_all(id_copies(1))

        @pl.when(i >= 1)
        def _():
            core_add(2 * i - 2)
            core_add(2 * i - 1)

        @pl.when(i == 1)
        def _():
            start_all(a_copies(0))
            start_all(a_copies(1))

        @pl.when(i == 2)
        def _():
            start_all(a_copies(2))
            start_all(a_copies(3))

        pl.when(i == 3)(lambda: do_b(0))
        pl.when(i == 5)(lambda: do_b(1))

        @pl.when(i == 6)
        def _():
            do_b(2)
            do_f(0)
            start_all(a2_copies())

        return np_, nq_, lp_, lq_

    lax.fori_loop(0, STEPS // 2, first_product, tuple(jnp.int32(t) for t in (next_p, next_q, load_p, load_q)))

    def reduce_rows(acc, chunk, u):
        for h, slope in enumerate((slope_a, slope_b)):
            lanes = pl.ds(h * LANES, LANES)
            span = jnp.zeros((spans, LANES), jnp.float32)
            for client in range(clients):
                lines = pl.ds(client * spans, spans)
                grad = acc[lines, lanes] * slope[chunk, lines, :].astype(jnp.float32)
                span = span + grad
                sums[u, pl.ds(spans + client, 1), lanes] = jnp.sum(grad, axis=0, keepdims=True)
            sums[u, pl.ds(0, spans), lanes] = span

    for part in range(4):
        weight_copy(part).wait()

    def second_product(g, carry):
        before, table = carry
        chunk0 = lax.rem(y + lax.rem(table, 4), 4) * 4
        for t in range(4):
            u = 4 * g + t
            now, last = (acc_a, acc_b) if t % 2 == 0 else (acc_b, acc_a)
            chunk = chunk0 + t
            previous = before if t == 0 else chunk - 1
            slot = lax.rem(u + STEPS, STEPS + 1)
            reduce_rows(last, previous, slot)
            lines = pl.ds(pl.multiple_of(chunk * BLOCK, BLOCK), BLOCK)
            now[...] = lax.dot_general(low[...], weight[lines, :], (((1,), (1,)), ((), ())), preferred_element_type=jnp.float32)
            if t == 1:

                @pl.when(g == 0)
                def _():
                    core_add(STEPS - 2)
                    core_add(STEPS - 1)
                    do_b(3)
                    do_f(1)

                for group in range(3):

                    @pl.when(g == group + 1)
                    def _(group=group):
                        send_spans(group, 1)
                        for k in range(4):
                            rows_low[group, k] = sums[4 * group + k, pl.ds(spans, clients), :].astype(jnp.bfloat16)
                        y_rows(group).start()

                @pl.when(g == 1)
                def _():
                    do_f(2)
                    do_b2()

                pl.when(g == 2)(lambda: do_f(3))
            elif t == 3:
                for group in range(3):
                    pl.when(g == group)(lambda group=group: send_spans(group, 0))
                pl.when(g == 2)(do_final)
        return chunk0 + 3, lax.div(table, 4)

    final_chunk, _ = lax.fori_loop(0, 4, second_product, (jnp.int32(0), jnp.int32(digits(YORDER))))
    reduce_rows(acc_b, final_chunk, STEPS - 1)

    half_here = here // 2
    for t in range(2):
        lanes = pl.ds(pl.multiple_of((1 - c) * half_here + t * BLOCK, BLOCK), BLOCK)
        own_send[t, pl.ds(0, spans), :] = sums[12 + 2 * (1 - c) + t, pl.ds(0, spans), :].astype(jnp.bfloat16)
        own_send[t, pl.ds(spans, 16), :] = bias_rows[:, lanes].astype(jnp.bfloat16)
    own_copy().start()
    for group in range(3):
        y_rows(group).wait_recv()
        for core in range(2):
            y_arrival(group, core).wait_recv()
    embed_square = jnp.zeros((1, LANES), jnp.float32)
    for t in range(4):
        mine = sums[12 + t, pl.ds(spans, clients), :]
        for group in range(3):
            mine = mine + rows_in[group, t].astype(jnp.float32)
        emb[0, 0, :, pl.ds(t * BLOCK, BLOCK)] = mine.astype(jnp.bfloat16)
        square = jnp.sum(mine * mine, axis=0, keepdims=True)
        embed_square = embed_square + square[:, :LANES] + square[:, LANES:]
    own_copy().wait_recv()
    for t in range(2):
        total = sums[12 + 2 * c + t, pl.ds(0, spans), :] + own_in[t, pl.ds(0, spans), :].astype(jnp.float32)
        for group in range(3):
            for core in range(2):
                total = total + span_in[group, core, t].astype(jnp.float32)
        lanes = pl.ds(t * BLOCK, BLOCK)
        rest_own[pl.ds(0, spans), lanes] = total.astype(jnp.bfloat16)
        mine = bias_rows[:, pl.ds(pl.multiple_of(c * half_here + t * BLOCK, BLOCK), BLOCK)]
        rest_own[pl.ds(spans, 16), lanes] = (mine + own_in[t, pl.ds(spans, 16), :].astype(jnp.float32)).astype(jnp.bfloat16)
    squares[0, pl.ds(1, 1), :] = embed_square
    over(1, 16, lambda o: scatter_copy(o).start())
    start_all(embed_copies(0))
    over(1, 16, lambda o: scatter_copy(o).wait_recv())
    piece = rest_own[piece_of(z, x)].astype(jnp.float32)
    piece = piece + jnp.sum(rest_in[1:].astype(jnp.float32), axis=0)
    rest_all[piece_of(z, c * 4 + x)] = piece.astype(jnp.bfloat16)
    squares[0, pl.ds(2, 1), :] = jnp.sum(piece * piece, axis=0, keepdims=True)
    over(1, 32, lambda o: gather_copy(o).start())
    over(1, 16, lambda o: plane_copy(o).start())
    arrive_all(embed_copies(0))
    start_all(embed_copies(1))
    over(1, 16, lambda o: plane_copy(o).wait_recv())
    squares[1] = squares[0] + jnp.sum(squares_zx[1:], axis=0)
    over(1, 8, lambda o: column_copy(o).start())
    over(1, 32, lambda o: gather_copy(o).wait_recv())
    arrive_all(id_copies(1))
    lane = lax.broadcasted_iota(jnp.int32, (1, LANES), 1)
    chip = (z * 4 + x) * 2
    wanted = jnp.where(lane < clients, (chip + c) * clients + lane, jnp.where(lane < 2 * clients, (chip + 1 - c) * clients + lane - clients, -1))
    chosen = (ids[...].reshape(16 * clients, LANES) == wanted).astype(jnp.float32).astype(jnp.bfloat16)
    arrive_all(embed_copies(1))
    table = lax.dot_general(chosen, emb[...].reshape(16 * clients, here), (((0,), (0,)), ((), ())), preferred_element_type=jnp.float32)
    picked[...] = table[clients : 2 * clients].astype(jnp.bfloat16)
    picked_copy().start()
    over(1, 8, lambda o: column_copy(o).wait_recv())
    total_out[...] = squares[1] + jnp.sum(squares_y[1:], axis=0)
    rest_out[...] = rest_all[pl.ds(0, spans + 16), :]
    picked_copy().wait_recv()
    embed_out[...] = table[:clients] + picked_in[...].astype(jnp.float32)

    over(0, STEPS, lambda s: core_copy(s).wait_send())
    sent = [*a2_copies(), *b2_copies(), picked_copy(), own_copy()]
    for i in range(4):
        sent += [*a_copies(i), *b_copies(i)]
    for group in range(3):
        sent += [y_rows(group), y_spans(group, 0), y_spans(group, 1)]
    for k in range(2):
        sent += [*id_copies(k), *embed_copies(k)]
    for copy in sent:
        copy.wait_send()
    over(1, 16, lambda o: scatter_copy(o).wait_send())
    over(1, 32, lambda o: gather_copy(o).wait_send())
    over(1, 16, lambda o: plane_copy(o).wait_send())
    over(1, 8, lambda o: column_copy(o).wait_send())


def scale(head, rest, embed, total, head_out, bias_out, embed_out, span_out):
    spans, here = span_out.shape
    width, emit = here * 4, here * 4

    def factor(line, number):
        whole = jnp.sum(total[pl.ds(line, 1), :], axis=1, keepdims=True)
        return jnp.minimum(1.0, 1.0 / jnp.sqrt(whole / number + EPSILON))

    head_out[...] = head[...] * factor(0, width * emit)
    embed_out[...] = embed[...] * factor(1, 32 * embed.shape[0] * width)
    small = factor(2, spans * width + emit)
    span_out[...] = rest[pl.ds(0, spans), :].astype(jnp.float32) * small
    bias_out[...] = rest[pl.ds(spans, 16), :].astype(jnp.float32)[:1] * small


def per_device(pre, delta, head_weight, client_ids):
    rows, width = pre.shape
    here = delta.shape[1]
    clients = client_ids.shape[0]
    bf16, f32 = jnp.bfloat16, jnp.float32
    dma = pltpu.SemaphoreType.DMA
    spans = rows // clients
    anywhere = pl.BlockSpec(memory_space=pl.ANY)
    in_vmem = pl.BlockSpec(memory_space=pltpu.VMEM)
    head, rest, embed, total = pl.pallas_call(
        kernel,
        name="products",
        out_shape=(
            jax.ShapeDtypeStruct((LANES, here), f32),
            jax.ShapeDtypeStruct((spans + 16, here), bf16),
            jax.ShapeDtypeStruct((clients, here), f32),
            jax.ShapeDtypeStruct((8, LANES), f32),
        ),
        in_specs=[anywhere] * 3 + [pl.BlockSpec(memory_space=pltpu.SMEM)],
        out_specs=[in_vmem] * 4,
        scratch_shapes=[
            pltpu.VMEM((3, 256, here), f32),
            pltpu.VMEM((rows, here), bf16),
            pltpu.VMEM((here, rows), bf16),
            pltpu.VMEM((width, here), bf16),
            pltpu.VMEM((4, rows, BLOCK), bf16),
            pltpu.VMEM((rows, BLOCK), bf16),
            pltpu.VMEM((rows, BLOCK), bf16),
            pltpu.VMEM((STEPS + 1, rows, LANES), bf16),
            pltpu.VMEM((STEPS + 1, rows, LANES), bf16),
            pltpu.VMEM((STEPS, 2, here, LANES), bf16),
            pltpu.VMEM((STEPS, here, LANES), bf16),
            pltpu.VMEM((rows, BLOCK), f32),
            pltpu.VMEM((rows, BLOCK), f32),
            pltpu.VMEM((STEPS + 1, spans + 16, BLOCK), f32),
            pltpu.VMEM((12, spans, BLOCK), bf16),
            pltpu.VMEM((3, 4, clients, BLOCK), bf16),
            pltpu.VMEM((3, 2, 2, spans, BLOCK), bf16),
            pltpu.VMEM((3, 4, clients, BLOCK), bf16),
            pltpu.VMEM((2, spans + 16, BLOCK), bf16),
            pltpu.VMEM((2, spans + 16, BLOCK), bf16),
            pltpu.VMEM((16, here), f32),
            pltpu.VMEM((4, 2, here // 2, LANES), bf16),
            pltpu.VMEM((4, 2, here, LANES), bf16),
            pltpu.VMEM((2, here // 2, LANES), bf16),
            pltpu.VMEM((2, here, LANES), bf16),
            pltpu.VMEM((4, 4, clients, LANES), jnp.int32),
            pltpu.VMEM((4, 4, clients, here), bf16),
            pltpu.VMEM((128, here // 2), bf16),
            pltpu.VMEM((16, 32, LANES), bf16),
            pltpu.VMEM((128, here), bf16),
            pltpu.VMEM((clients, here), bf16),
            pltpu.VMEM((clients, here), bf16),
            pltpu.VMEM((2, 8, LANES), f32),
            pltpu.VMEM((16, 8, LANES), f32),
            pltpu.VMEM((8, 8, LANES), f32),
            dma((3,)),
            dma((4,)),
            dma((4, 2)),
            *[dma((STEPS,))] * 2,
            *[dma((4, 2))] * 2,
            *[dma((4, 4))] * 2,
            *[dma((2,))] * 2,
            *[dma((4,))] * 2,
            *[dma((3,))] * 2,
            *[dma((3, 2))] * 2,
            dma((2,)),
            *[dma((2, 4))] * 4,
            *[dma((16,))] * 2,
            *[dma((32,))] * 2,
            *[dma((1,))] * 2,
            *[dma((16,))] * 2,
            *[dma((8,))] * 2,
        ],
        compiler_params=pltpu.CompilerParams(collective_id=0, has_side_effects=True, vmem_limit_bytes=67_000_000),
    )(pre, delta, head_weight, client_ids)
    head, bias, embed, span = pl.pallas_call(
        scale,
        name="scale",
        out_shape=(
            jax.ShapeDtypeStruct((LANES, here), f32),
            jax.ShapeDtypeStruct((1, here), f32),
            jax.ShapeDtypeStruct((clients, here), f32),
            jax.ShapeDtypeStruct((spans, here), f32),
        ),
        in_specs=[in_vmem] * 4,
        out_specs=[in_vmem] * 4,
    )(head, rest, embed, total)
    return head, bias[0], embed, span


def solution(mesh):
    torus = Mesh(
        mesh.devices.reshape(4, 4, 2, mesh.shape["head"]),
        ("client_0", "client_1", "client_2", "head"),
    )
    return jax.shard_map(
        per_device,
        mesh=torus,
        in_specs=(P(CLIENT, None), P(CLIENT, "head"), P(None, "head"), P(CLIENT)),
        out_specs=(P(CLIENT, "head"), P("head"), P(CLIENT, "head"), P(None, "head")),
        check_vma=False,
    )
```
